8 devices in a mesh: dp: 1 (over z), sp: 8 (over y, x, core).
Axes of the slice: x: 2, y: 2, z: 1, core: 2. Of those that a mesh axis runs over, the one named last changes fastest.
Arguments:
- x_in: bfloat16 [1, 8192, 3840], P('dp', 'sp')
- dy_in: bfloat16 [1, 8192, 3840], P('dp', 'sp')
- positions: int32 [8192], P(('dp', 'sp'))
- w_q: bfloat16 [3840, 4096], replicated
- w_k: bfloat16 [3840, 2048], replicated
- w_v: bfloat16 [3840, 2048], replicated
- w_o: bfloat16 [4096, 3840], replicated
- w_pre: float32 [3840], replicated
- w_post: float32 [3840], replicated
- q_norm: float32 [256], replicated
- k_norm: float32 [256], replicated
Outputs:
- output 1: bfloat16 [1, 8192, 3840], P('dp', 'sp')
- output 2: bfloat16 [1, 8192, 3840], P('dp', 'sp')
- output 3: bfloat16 [3840, 4096], P('dp')
- output 4: bfloat16 [3840, 2048], P('dp')
- output 5: bfloat16 [3840, 2048], P('dp')
- output 6: bfloat16 [4096, 3840], P('dp')
- output 7: float32 [3840], P('dp')
- output 8: float32 [3840], P('dp')
- output 9: float32 [256], P('dp')
- output 10: float32 [256], P('dp')
All inputs are finite; a program needn't handle non-finite values.
Results may differ from the reference program's by a relative error of at most 0.02.
Values are sent between devices in bfloat16 or wider.
A program may use at most 1 GiB of HBM per device.

```python
import functools
import jax
import jax.numpy as jnp
from jax import lax

B = 1
SEQ = 8192
D = 3840
H = 16
K = 8
HEAD = 256

EPS = 1e-6
ROPE_BASE = 1000000.0
ROPE_SCALE = 8.0
NEG_BIG = -1e30
Q_ROWS = min(128, SEQ)


def setup_inputs(seed: int = 0, part: int = 0) -> dict:
    base_key = jax.random.key(seed)
    own = jax.random.split(jax.random.fold_in(base_key, part), 4)
    shared = jax.random.split(base_key, 8)
    x_in = jax.random.normal(own[0], (B, SEQ, D), jnp.float32).astype(jnp.bfloat16)
    dy_in = jax.random.normal(own[1], (B, SEQ, D), jnp.float32).astype(jnp.bfloat16)
    start = jax.random.randint(own[2], (1,), 0, 1000)
    gaps = jax.random.randint(own[3], (SEQ,), 1, 5)
    positions = (start + jnp.cumsum(gaps) - gaps[0]).astype(jnp.int32)
    w_q = (jax.random.normal(shared[0], (D, H * HEAD), jnp.float32) * D ** -0.5).astype(jnp.bfloat16)
    w_k = (jax.random.normal(shared[1], (D, K * HEAD), jnp.float32) * D ** -0.5).astype(jnp.bfloat16)
    w_v = (jax.random.normal(shared[2], (D, K * HEAD), jnp.float32) * D ** -0.5).astype(jnp.bfloat16)
    w_o = (jax.random.normal(shared[3], (H * HEAD, D), jnp.float32) * (H * HEAD) ** -0.5).astype(jnp.bfloat16)
    w_pre = 0.3 * jax.random.normal(shared[4], (D,), jnp.float32)
    w_post = 0.3 * jax.random.normal(shared[5], (D,), jnp.float32)
    q_norm = 0.3 + 0.3 * jax.random.normal(shared[6], (HEAD,), jnp.float32)
    k_norm = 0.3 + 0.3 * jax.random.normal(shared[7], (HEAD,), jnp.float32)
    return {'x_in': x_in, 'dy_in': dy_in, 'positions': positions, 'w_q': w_q, 'w_k': w_k, 'w_v': w_v, 'w_o': w_o, 'w_pre': w_pre, 'w_post': w_post, 'q_norm': q_norm, 'k_norm': k_norm}


def rms_scale(x_f32, weight):
    inv_rms = lax.rsqrt(jnp.mean(x_f32 * x_f32, axis=-1, keepdims=True) + EPS)
    return x_f32 * inv_rms * (1.0 + weight)


def norm_rope(heads_f32, weight, cosines, sines):
    half_dim = HEAD // 2
    normed = rms_scale(heads_f32, weight)
    first = normed[..., :half_dim]
    second = normed[..., half_dim:]
    cos_b = cosines[None, :, None, :]
    sin_b = sines[None, :, None, :]
    return jnp.concatenate([first * cos_b - second * sin_b, second * cos_b + first * sin_b], axis=-1)


def attention(q_rot, k_rot, v_heads):
    group = H // K
    blocks = SEQ // Q_ROWS
    q_blocks = jnp.moveaxis(q_rot.reshape(B, blocks, Q_ROWS, K, group, HEAD), 1, 0)
    key_f32 = k_rot.astype(jnp.float32)
    val_f32 = v_heads.astype(jnp.float32)
    col_ids = jnp.arange(SEQ)

    def one_block(item):
        q_blk, index = item
        scores = jnp.einsum('bqkgh,bskh->bkgqs', q_blk.astype(jnp.float32), key_f32) * HEAD ** -0.5
        row_ids = index * Q_ROWS + jnp.arange(Q_ROWS)
        scores = jnp.where(row_ids[:, None] >= col_ids[None, :], scores, NEG_BIG)
        attn_prob = jax.nn.softmax(scores, axis=-1).astype(jnp.bfloat16).astype(jnp.float32)
        return jnp.einsum('bkgqs,bskh->bqkgh', attn_prob, val_f32).astype(jnp.bfloat16)

    block_out = lax.map(jax.checkpoint(one_block), (q_blocks, jnp.arange(blocks)))
    return jnp.moveaxis(block_out, 0, 1).reshape(B, SEQ, H, HEAD)


def forward(positions, x_in, w_q, w_k, w_v, w_o, w_pre, w_post, q_norm, k_norm):
    x_f32 = x_in.astype(jnp.float32)
    normed = rms_scale(x_f32, w_pre).astype(jnp.bfloat16).astype(jnp.float32)
    q_proj = jnp.einsum('bsd,dn->bsn', normed, w_q.astype(jnp.float32)).astype(jnp.bfloat16)
    k_proj = jnp.einsum('bsd,dn->bsn', normed, w_k.astype(jnp.float32)).astype(jnp.bfloat16)
    v_proj = jnp.einsum('bsd,dn->bsn', normed, w_v.astype(jnp.float32)).astype(jnp.bfloat16)
    half_dim = HEAD // 2
    inv_freq = ROPE_BASE ** (-jnp.arange(half_dim, dtype=jnp.float32) * 2.0 / HEAD)
    angles = (positions.astype(jnp.float32) / ROPE_SCALE)[:, None] * inv_freq[None, :]
    cosines = jnp.cos(angles)
    sines = jnp.sin(angles)
    q_rot = norm_rope(q_proj.reshape(B, SEQ, H, HEAD).astype(jnp.float32), q_norm, cosines, sines).astype(jnp.bfloat16)
    k_rot = norm_rope(k_proj.reshape(B, SEQ, K, HEAD).astype(jnp.float32), k_norm, cosines, sines).astype(jnp.bfloat16)
    v_heads = v_proj.reshape(B, SEQ, K, HEAD)
    attn_out = attention(q_rot, k_rot, v_heads)
    proj = jnp.einsum('bsn,nd->bsd', attn_out.reshape(B, SEQ, H * HEAD).astype(jnp.float32), w_o.astype(jnp.float32)).astype(jnp.bfloat16)
    return (x_f32 + rms_scale(proj.astype(jnp.float32), w_post)).astype(jnp.bfloat16)


def reference(x_in, dy_in, positions, w_q, w_k, w_v, w_o, w_pre, w_post, q_norm, k_norm):
    y_out, pullback = jax.vjp(functools.partial(forward, positions), x_in, w_q, w_k, w_v, w_o, w_pre, w_post, q_norm, k_norm)
    grads = pullback(dy_in)
    return (y_out, grads[0], grads[1], grads[2], grads[3], grads[4], grads[5], grads[6], grads[7], grads[8])
```

```python
import functools
import math
import jax
import jax.numpy as jnp
from jax import lax
from jax.experimental import pallas as pl
from jax.experimental.pallas import tpu as pltpu
from jax.sharding import PartitionSpec as P

EPS = 1e-6
ROPE_BASE = 1000000.0
ROPE_SCALE = 8.0
NEG_BIG = -1e30
LOG2E = 1.4426950408889634
F32 = jnp.float32
BF16 = jnp.bfloat16
NT = (((1,), (1,)), ((), ()))
NN = (((1,), (0,)), ((), ()))
TN = (((0,), (0,)), ((), ()))
VMEM_LIMIT = 60 * 1024 * 1024


def dot(a, b, dims):
    return lax.dot_general(a, b, dims, preferred_element_type=F32)


def rms_scale(x_f32, weight):
    inv_rms = lax.rsqrt(jnp.mean(x_f32 * x_f32, axis=-1, keepdims=True) + EPS)
    return x_f32 * inv_rms * (1.0 + weight)


def pre_norm(x_f32, weight):
    return rms_scale(x_f32, weight).astype(BF16)


def post_norm(proj, weight):
    return rms_scale(proj.astype(F32), weight)


def rope_tables(positions, head):
    half_dim = head // 2
    inv_freq = ROPE_BASE ** (-jnp.arange(half_dim, dtype=F32) * 2.0 / head)
    angles = (positions.astype(F32) / ROPE_SCALE)[:, None] * inv_freq[None, :]
    return jnp.cos(angles), jnp.sin(angles)


def rope_fwd_kernel(n_q, n_k, head, x_ref, cos_ref, sin_ref, wq_ref, wk_ref, q_ref, k_ref):
    half = head // 2
    cosines = cos_ref[...]
    sines = sin_ref[...]
    for h in range(n_q + n_k):
        x = x_ref[:, h * head:(h + 1) * head].astype(F32)
        w_ref, out_ref, at = (wq_ref, q_ref, h) if h < n_q else (wk_ref, k_ref, h - n_q)
        normed = rms_scale(x, w_ref[...])
        first = normed[:, :half]
        second = normed[:, half:]
        out_ref[:, at * head:at * head + half] = (first * cosines - second * sines).astype(BF16)
        out_ref[:, at * head + half:(at + 1) * head] = (second * cosines + first * sines).astype(BF16)


def rope_fwd(qkv, cosines, sines, w_qn, w_kn, n_q, n_k, head):
    seq = qkv.shape[0]
    rows = min(512, seq)
    half = head // 2
    row = lambda width: pl.BlockSpec((rows, width), lambda i: (i, 0))
    whole = pl.BlockSpec((1, head), lambda i: (0, 0))
    return pl.pallas_call(
        functools.partial(rope_fwd_kernel, n_q, n_k, head),
        name='rope_fwd',
        grid=(seq // rows,),
        in_specs=[row((n_q + n_k) * head), row(half), row(half), whole, whole],
        out_specs=[row(n_q * head), row(n_k * head)],
        out_shape=[jax.ShapeDtypeStruct((seq, n_q * head), BF16), jax.ShapeDtypeStruct((seq, n_k * head), BF16)],
        compiler_params=pltpu.CompilerParams(dimension_semantics=('arbitrary',)),
        cost_estimate=pl.CostEstimate(flops=seq * (n_q + n_k) * head * 12, bytes_accessed=seq * (n_q + n_k) * head * 4 + seq * head * 4, transcendentals=0),
    )(qkv, cosines, sines, w_qn, w_kn)


def rope_bwd_kernel(n_q, n_k, head, dq_ref, dk_ref, x_ref, cos_ref, sin_ref, wq_ref, wk_ref, oq_ref, ok_ref, gq_ref, gk_ref):
    half = head // 2
    cosines = cos_ref[...]
    sines = sin_ref[...]

    @pl.when(pl.program_id(0) == 0)
    def _():
        gq_ref[...] = jnp.zeros_like(gq_ref)
        gk_ref[...] = jnp.zeros_like(gk_ref)

    for h in range(n_q + n_k):
        x = x_ref[:, h * head:(h + 1) * head].astype(F32)
        g_in, w_ref, out_ref, sum_ref, at = (dq_ref, wq_ref, oq_ref, gq_ref, h) if h < n_q else (dk_ref, wk_ref, ok_ref, gk_ref, h - n_q)
        d_first = g_in[:, at * head:at * head + half].astype(F32)
        d_second = g_in[:, at * head + half:(at + 1) * head].astype(F32)
        g = jnp.concatenate([d_first * cosines + d_second * sines, d_second * cosines - d_first * sines], axis=1)
        inv_rms = lax.rsqrt(jnp.mean(x * x, axis=-1, keepdims=True) + EPS)
        x_hat = x * inv_rms
        rows = x.shape[0]
        sum_ref[...] += jnp.sum((g * x_hat).reshape(rows // 8, 8, head), axis=0)
        gw = g * (1.0 + w_ref[...])
        out = inv_rms * (gw - x_hat * jnp.mean(gw * x_hat, axis=-1, keepdims=True))
        out_ref[:, at * head:(at + 1) * head] = out.astype(BF16)


def rope_bwd(dq, dk, qkv, cosines, sines, w_qn, w_kn, n_q, n_k, head):
    seq = qkv.shape[0]
    rows = min(512, seq)
    half = head // 2
    row = lambda width: pl.BlockSpec((rows, width), lambda i: (i, 0))
    whole = pl.BlockSpec((1, head), lambda i: (0, 0))
    sums = pl.BlockSpec((8, head), lambda i: (0, 0))
    return pl.pallas_call(
        functools.partial(rope_bwd_kernel, n_q, n_k, head),
        name='rope_bwd',
        grid=(seq // rows,),
        in_specs=[row(n_q * head), row(n_k * head), row((n_q + n_k) * head), row(half), row(half), whole, whole],
        out_specs=[row(n_q * head), row(n_k * head), sums, sums],
        out_shape=[jax.ShapeDtypeStruct((seq, n_q * head), BF16), jax.ShapeDtypeStruct((seq, n_k * head), BF16),
                   jax.ShapeDtypeStruct((8, head), F32), jax.ShapeDtypeStruct((8, head), F32)],
        compiler_params=pltpu.CompilerParams(dimension_semantics=('arbitrary',)),
        cost_estimate=pl.CostEstimate(flops=seq * (n_q + n_k) * head * 20, bytes_accessed=seq * (n_q + n_k) * head * 6 + seq * head * 4, transcendentals=0),
    )(dq, dk, qkv, cosines, sines, w_qn, w_kn)


BQ = 512
BK = 512


def attn_fwd_kernel(per, head, blk, q_ref, k_ref, v_ref, o_ref, lse_ref, m_sc, l_sc, acc_sc):
    i = pl.program_id(0)
    c = LOG2E * head ** -0.5
    m_sc[...] = jnp.full_like(m_sc, -jnp.inf)
    l_sc[...] = jnp.zeros_like(l_sc)
    acc_sc[...] = jnp.zeros_like(acc_sc)

    def step(j, masked):
        at = pl.multiple_of(j * blk, blk)
        k = k_ref[pl.ds(at, blk), :]
        v = v_ref[pl.ds(at, blk), :]
        for h in range(per):
            s = dot(q_ref[:, h * head:(h + 1) * head], k, NT)
            if masked:
                rows = lax.broadcasted_iota(jnp.int32, s.shape, 0)
                cols = lax.broadcasted_iota(jnp.int32, s.shape, 1)
                s = jnp.where(rows >= cols, s, NEG_BIG)
            t = s * c
            m_prev = m_sc[h]
            m_new = jnp.maximum(m_prev, jnp.max(t, axis=1, keepdims=True))
            m_sc[h] = m_new
            p = jnp.exp2(t - jnp.tile(m_new, (1, blk // 128)))
            alpha = jnp.exp2(m_prev - m_new)
            part = p[:, :128]
            for z in range(1, blk // 128):
                part = part + p[:, z * 128:(z + 1) * 128]
            l_sc[h] = l_sc[h] * alpha + part
            acc_sc[h] = acc_sc[h] * jnp.tile(alpha, (1, head // 128)) + dot(p.astype(BF16), v, NN)

    @pl.loop(0, i)
    def _(j):
        step(j, False)

    step(i, True)
    for h in range(per):
        total = jnp.sum(l_sc[h], axis=1, keepdims=True)
        o_ref[:, h * head:(h + 1) * head] = (acc_sc[h] / total).astype(BF16)
        lse = m_sc[h] + jnp.log2(jnp.broadcast_to(total, (blk, 128)))
        lse_ref[h:h + 1, :] = lse.T[0:1, :]


def attn_fwd(q, k, v, per, head):
    seq = q.shape[0]
    blk = min(BQ, seq)
    pairs = seq * (seq + blk) // 2 * per
    row = pl.BlockSpec((blk, per * head), lambda i: (i, 0))
    whole = pl.BlockSpec((seq, head), lambda i: (0, 0))
    return pl.pallas_call(
        functools.partial(attn_fwd_kernel, per, head, blk),
        name='attn_fwd',
        grid=(seq // blk,),
        in_specs=[row, whole, whole],
        out_specs=[row, pl.BlockSpec((per, blk), lambda i: (0, i))],
        out_shape=[jax.ShapeDtypeStruct((seq, per * head), BF16), jax.ShapeDtypeStruct((per, seq), F32)],
        scratch_shapes=[pltpu.VMEM((per, blk, 128), F32), pltpu.VMEM((per, blk, 128), F32), pltpu.VMEM((per, blk, head), F32)],
        compiler_params=pltpu.CompilerParams(dimension_semantics=('arbitrary',), vmem_limit_bytes=VMEM_LIMIT),
        cost_estimate=pl.CostEstimate(flops=4 * pairs * head, bytes_accessed=seq * head * 2 * (2 * per + 2), transcendentals=pairs),
    )(q, k, v)


def attn_bwd_kernel(per, head, blk, q_ref, do_ref, o_ref, lse_ref, k_ref, v_ref, dq_ref, dk_ref, dv_ref, dk_acc, dv_acc, dq_acc, q_sc, do_sc, delta_sc):
    i = pl.program_id(0)
    last = pl.num_programs(0) - 1
    scale = head ** -0.5
    c = LOG2E * scale
    for h in range(per):
        lanes = slice(h * head, (h + 1) * head)
        rows = slice(h * blk, (h + 1) * blk)
        q_sc[rows, :] = q_ref[:, lanes]
        do_sc[rows, :] = do_ref[:, lanes]
        prod = do_ref[:, lanes].astype(F32) * o_ref[:, lanes].astype(F32)
        delta = jnp.broadcast_to(jnp.sum(prod, axis=1, keepdims=True), (blk, 128))
        delta_sc[:, rows] = delta.T[0:1, :]

    def step(j, diag):
        at = pl.multiple_of(j * blk, blk)
        k = k_ref[pl.ds(at, blk), :]
        v = v_ref[pl.ds(at, blk), :]
        dvs = []
        dks = []
        dqs = []
        for h in range(per):
            rows = slice(h * blk, (h + 1) * blk)
            q = q_sc[rows, :]
            d_out = do_sc[rows, :]
            s = dot(k, q, NT)
            p = jnp.exp2(s * c - lse_ref[h:h + 1, :])
            if diag:
                kv_ids = lax.broadcasted_iota(jnp.int32, s.shape, 0)
                q_ids = lax.broadcasted_iota(jnp.int32, s.shape, 1)
                p = jnp.where(q_ids >= kv_ids, p, 0.0)
            dp = dot(v, d_out, NT)
            ds = (p * (dp - delta_sc[:, rows])).astype(BF16)
            dvs.append(dot(p.astype(BF16), d_out, NN))
            dks.append(dot(ds, q, NN))
            dqs.append(dot(ds, k, TN))
        d_v = functools.reduce(jnp.add, dvs)
        d_k = functools.reduce(jnp.add, dks)
        if diag:
            dv_acc[pl.ds(at, blk), :] = d_v
            dk_acc[pl.ds(at, blk), :] = d_k
        else:
            dv_acc[pl.ds(at, blk), :] += d_v
            dk_acc[pl.ds(at, blk), :] += d_k
        for h in range(per):
            rows = slice(h * blk, (h + 1) * blk)
            if diag:
                dq_acc[rows, :] = dqs[h]
            else:
                dq_acc[rows, :] += dqs[h]

    step(i, True)

    @pl.loop(0, i)
    def _(j):
        step(j, False)

    for h in range(per):
        dq_ref[:, h * head:(h + 1) * head] = (dq_acc[h * blk:(h + 1) * blk, :] * scale).astype(BF16)

    @pl.when(i == last)
    def _():
        @pl.loop(0, dk_acc.shape[0] // blk)
        def _(j):
            at = pl.ds(pl.multiple_of(j * blk, blk), blk)
            dk_ref[at, :] = (dk_acc[at, :] * scale).astype(BF16)
            dv_ref[at, :] = dv_acc[at, :].astype(BF16)


def attn_bwd(q, d_out, o, lse, k, v, per, head):
    seq = q.shape[0]
    blk = min(BQ, seq)
    pairs = seq * (seq + blk) // 2 * per
    row = pl.BlockSpec((blk, per * head), lambda i: (i, 0))
    whole = pl.BlockSpec((seq, head), lambda i: (0, 0), pipeline_mode=pl.Buffered(1))
    return pl.pallas_call(
        functools.partial(attn_bwd_kernel, per, head, blk),
        name='attn_bwd',
        grid=(seq // blk,),
        in_specs=[row, row, row, pl.BlockSpec((per, blk), lambda i: (0, i)), whole, whole],
        out_specs=[row, whole, whole],
        out_shape=[jax.ShapeDtypeStruct((seq, per * head), BF16), jax.ShapeDtypeStruct((seq, head), BF16), jax.ShapeDtypeStruct((seq, head), BF16)],
        scratch_shapes=[pltpu.VMEM((seq, head), F32), pltpu.VMEM((seq, head), F32), pltpu.VMEM((per * blk, head), F32),
                        pltpu.VMEM((per * blk, head), BF16), pltpu.VMEM((per * blk, head), BF16), pltpu.VMEM((1, per * blk), F32)],
        compiler_params=pltpu.CompilerParams(dimension_semantics=('arbitrary',), vmem_limit_bytes=VMEM_LIMIT),
        cost_estimate=pl.CostEstimate(flops=10 * pairs * head, bytes_accessed=seq * head * 2 * (4 * per + 4), transcendentals=pairs),
    )(q, d_out, o, lse, k, v)


def solution(mesh):
    group = mesh.shape['sp']

    def gather(arr, axis=0):
        return lax.all_gather(arr, 'sp', axis=axis, tiled=True)

    def device_step(x_in, dy_in, positions, w_q, w_k, w_v, w_o, w_pre, w_post, q_norm, k_norm):
        batch, seq_loc, width = x_in.shape
        head = q_norm.shape[0]
        n_q = w_q.shape[1] // head // group
        n_k = w_k.shape[1] // head // group
        me = lax.axis_index('sp')
        x_f32 = x_in[0].astype(F32)
        normed, pre_pull = jax.vjp(pre_norm, x_f32, w_pre)
        normed_all = gather(normed)
        cosines, sines = rope_tables(gather(positions), head)
        wq_mine = lax.dynamic_slice_in_dim(w_q, me * n_q * head, n_q * head, 1)
        wk_mine = lax.dynamic_slice_in_dim(w_k, me * n_k * head, n_k * head, 1)
        wv_mine = lax.dynamic_slice_in_dim(w_v, me * n_k * head, n_k * head, 1)
        qk = dot(normed_all, jnp.concatenate([wq_mine, wk_mine], axis=1), NN).astype(BF16)
        v_all = dot(normed_all, wv_mine, NN).astype(BF16)
        qn = q_norm[None, :]
        kn = k_norm[None, :]
        q_all, k_all = rope_fwd(qk, cosines, sines, qn, kn, n_q, n_k, head)
        o_all, lse = attn_fwd(q_all, k_all, v_all, n_q // n_k, head)
        o_flat = lax.all_to_all(o_all, 'sp', 0, 1, tiled=True)
        proj = dot(o_flat, w_o, NN).astype(BF16)
        post, post_pull = jax.vjp(post_norm, proj, w_post)
        y_out = (x_f32 + post).astype(BF16)
        dy_f32 = dy_in[0].astype(F32)
        d_proj, dw_post = post_pull(dy_f32)
        d_proj_all = gather(d_proj)
        wo_mine = lax.dynamic_slice_in_dim(w_o, me * n_q * head, n_q * head, 0)
        do_all = dot(d_proj_all, wo_mine, NT).astype(BF16)
        dw_o = gather(dot(o_all, d_proj_all, TN).astype(BF16))
        dq_all, dk_all, dv_all = attn_bwd(q_all, do_all, o_all, lse, k_all, v_all, n_q // n_k, head)
        dq_proj, dk_proj, gq, gk = rope_bwd(dq_all, dk_all, qk, cosines, sines, qn, kn, n_q, n_k, head)
        dq_flat = lax.all_to_all(dq_proj, 'sp', 0, 1, tiled=True)
        dk_flat = lax.all_to_all(dk_proj, 'sp', 0, 1, tiled=True)
        dv_flat = lax.all_to_all(dv_all, 'sp', 0, 1, tiled=True)
        dw_q = gather(dot(normed_all, dq_proj, TN).astype(BF16), 1)
        dw_k = gather(dot(normed_all, dk_proj, TN).astype(BF16), 1)
        dw_v = gather(dot(normed_all, dv_all, TN).astype(BF16), 1)
        d_normed = (dot(dq_flat, w_q, NT) + dot(dk_flat, w_k, NT) + dot(dv_flat, w_v, NT)).astype(BF16)
        dx_norm, dw_pre = pre_pull(d_normed)
        dx_out = (dy_f32 + dx_norm).astype(BF16)
        sums = lax.psum((dw_pre, dw_post, jnp.sum(gq, axis=0), jnp.sum(gk, axis=0)), 'sp')
        return (y_out[None], dx_out[None], dw_q, dw_k, dw_v, dw_o, sums[0], sums[1], sums[2], sums[3])

    token_spec = P('dp', 'sp', None)
    return jax.shard_map(device_step, mesh=mesh,
                         in_specs=(token_spec, token_spec, P(('dp', 'sp')), P(None, None), P(None, None), P(None, None), P(None, None), P(None), P(None), P(None), P(None)),
                         out_specs=(token_spec, token_spec, P('dp', None), P('dp', None), P('dp', None), P('dp', None), P('dp'), P('dp'), P('dp'), P('dp')),
                         check_vma=False)
```

```python
import functools
import jax
import jax.numpy as jnp
from jax import lax
from jax.experimental import pallas as pl
from jax.experimental.pallas import tpu as pltpu
from jax.sharding import PartitionSpec as P

EPS = 1e-6
ROPE_BASE = 1000000.0
ROPE_SCALE = 8.0
NEG_BIG = -1e30
LOG2E = 1.4426950408889634
F32 = jnp.float32
BF16 = jnp.bfloat16
NT = (((1,), (1,)), ((), ()))
NN = (((1,), (0,)), ((), ()))
TN = (((0,), (0,)), ((), ()))
VMEM_LIMIT = 60 * 1024 * 1024


def dot(a, b, dims):
    return lax.dot_general(a, b, dims, preferred_element_type=F32)


def rms_scale(x_f32, weight):
    inv_rms = lax.rsqrt(jnp.mean(x_f32 * x_f32, axis=-1, keepdims=True) + EPS)
    return x_f32 * inv_rms * (1.0 + weight)


def pre_norm(x_f32, weight):
    return rms_scale(x_f32, weight).astype(BF16)


def post_norm(proj, weight):
    return rms_scale(proj.astype(F32), weight)


def rope_tables(positions, head):
    half_dim = head // 2
    inv_freq = ROPE_BASE ** (-jnp.arange(half_dim, dtype=F32) * 2.0 / head)
    angles = (positions.astype(F32) / ROPE_SCALE)[:, None] * inv_freq[None, :]
    return jnp.cos(angles), jnp.sin(angles)


def rope_fwd_kernel(n_q, n_k, head, x_ref, cos_ref, sin_ref, wq_ref, wk_ref, *refs):
    q_ref, k_ref, v_ref = refs[-3:]
    half = head // 2
    cosines = cos_ref[...]
    sines = sin_ref[...]
    for h in range(n_q + n_k):
        x = x_ref[:, h * head:(h + 1) * head].astype(F32)
        w_ref, out_ref, at = (wq_ref, q_ref, h) if h < n_q else (wk_ref, k_ref, h - n_q)
        normed = rms_scale(x, w_ref[...])
        first = normed[:, :half]
        second = normed[:, half:]
        out_ref[:, at * head:at * head + half] = (first * cosines - second * sines).astype(BF16)
        out_ref[:, at * head + half:(at + 1) * head] = (second * cosines + first * sines).astype(BF16)
    v_ref[...] = x_ref[:, (n_q + n_k) * head:]


def rope_fwd(z, qkv, cosines, sines, w_qn, w_kn, n_q, n_k, head, kv_so_far):
    seq = cosines.shape[0]
    blk = BLK
    half = head // 2
    row = lambda width: pl.BlockSpec((blk, width), lambda i: (i, 0))
    placed = lambda width: pl.BlockSpec((blk, width), lambda i: (2 * i + z, 0))
    whole = pl.BlockSpec((1, head), lambda i: (0, 0))
    kv_shape = jax.ShapeDtypeStruct((seq, n_k * head), BF16)
    return pl.pallas_call(
        functools.partial(rope_fwd_kernel, n_q, n_k, head),
        name='rope_fwd',
        grid=(qkv.shape[0] // blk,),
        in_specs=[row((n_q + 2 * n_k) * head), placed(half), placed(half), whole, whole] + [pl.BlockSpec(memory_space=pl.ANY)] * len(kv_so_far),
        out_specs=[row(n_q * head), placed(n_k * head), placed(n_k * head)],
        out_shape=[jax.ShapeDtypeStruct((qkv.shape[0], n_q * head), BF16), kv_shape, kv_shape],
        input_output_aliases={5: 1, 6: 2} if kv_so_far else {},
        compiler_params=pltpu.CompilerParams(dimension_semantics=('arbitrary',)),
        cost_estimate=pl.CostEstimate(flops=qkv.size * 40, bytes_accessed=qkv.size * 4 + seq * head * 2, transcendentals=0),
    )(qkv, cosines, sines, w_qn, w_kn, *kv_so_far)


def rope_bwd_kernel(n, head, d_ref, x_ref, cos_ref, sin_ref, w_ref, *refs):
    out_ref, sum_ref = refs[-2:]
    half = head // 2
    cosines = cos_ref[...]
    sines = sin_ref[...]

    @pl.when(pl.program_id(0) == 0)
    def _():
        sum_ref[...] = jnp.zeros_like(sum_ref)

    for h in range(n):
        x = x_ref[:, h * head:(h + 1) * head].astype(F32)
        d_first = d_ref[:, h * head:h * head + half].astype(F32)
        d_second = d_ref[:, h * head + half:(h + 1) * head].astype(F32)
        g = jnp.concatenate([d_first * cosines + d_second * sines, d_second * cosines - d_first * sines], axis=1)
        inv_rms = lax.rsqrt(jnp.mean(x * x, axis=-1, keepdims=True) + EPS)
        x_hat = x * inv_rms
        sum_ref[...] += jnp.sum((g * x_hat).reshape(x.shape[0] // 8, 8, head), axis=0)
        gw = g * (1.0 + w_ref[...])
        out = inv_rms * (gw - x_hat * jnp.mean(gw * x_hat, axis=-1, keepdims=True))
        out_ref[:, h * head:(h + 1) * head] = out.astype(BF16)
    if len(refs) == 3:
        out_ref[:, n * head:] = refs[0][...]


def rope_bwd(z, grad, beside, qkv, lane_block, cosines, sines, w_n, n, head):
    blk = BLK
    half = head // 2
    row = lambda width: pl.BlockSpec((blk, width), lambda i: (i, 0))
    placed = lambda width: pl.BlockSpec((blk, width), lambda i: (2 * i + z, 0))
    rows = qkv.shape[0]
    lanes = n * head + sum(b.shape[1] for b in beside)
    return pl.pallas_call(
        functools.partial(rope_bwd_kernel, n, head),
        name='rope_bwd',
        grid=(rows // blk,),
        in_specs=[placed(n * head) if beside else row(n * head), pl.BlockSpec((blk, n * head), lambda i: (i, lane_block)),
                  placed(half), placed(half), pl.BlockSpec((1, head), lambda i: (0, 0))] + [placed(b.shape[1]) for b in beside],
        out_specs=[row(lanes), pl.BlockSpec((8, head), lambda i: (0, 0))],
        out_shape=[jax.ShapeDtypeStruct((rows, lanes), BF16), jax.ShapeDtypeStruct((8, head), F32)],
        compiler_params=pltpu.CompilerParams(dimension_semantics=('arbitrary',)),
        cost_estimate=pl.CostEstimate(flops=rows * n * head * 60, bytes_accessed=rows * n * head * 6 + rows * head * 4, transcendentals=0),
    )(grad, qkv, cosines, sines, w_n, *beside)


def copy_kernel(x_ref, o_ref):
    o_ref[...] = x_ref[...]


def place(x):
    rows = 256
    spec = pl.BlockSpec((rows, x.shape[1]), lambda i: (i, 0))
    return pl.pallas_call(
        copy_kernel,
        name='place',
        grid=(x.shape[0] // rows,),
        in_specs=[spec],
        out_specs=spec,
        out_shape=jax.ShapeDtypeStruct(x.shape, x.dtype),
        compiler_params=pltpu.CompilerParams(dimension_semantics=('arbitrary',)),
        cost_estimate=pl.CostEstimate(flops=x.size * 16, bytes_accessed=4 * x.size, transcendentals=0),
    )(x)


BLK = 512


def attn_fwd_kernel(z, per, head, blk, q_ref, k_ref, v_ref, o_ref, lse_ref, m_sc, l_sc, acc_sc, s_even, s_odd):
    i = pl.program_id(0)
    c = LOG2E * head ** -0.5
    m_sc[...] = jnp.full_like(m_sc, -jnp.inf)
    l_sc[...] = jnp.zeros_like(l_sc)
    acc_sc[...] = jnp.zeros_like(acc_sc)

    def scores(j, s_ref):
        k = k_ref[pl.ds(pl.multiple_of(j * blk, blk), blk), :]
        for h in range(per):
            s_ref[h] = dot(q_ref[:, h * head:(h + 1) * head], k, NT)

    def update(j, s_ref, masked):
        v = v_ref[pl.ds(pl.multiple_of(j * blk, blk), blk), :]
        for h in range(per):
            s = s_ref[h]
            if masked:
                rows = lax.broadcasted_iota(jnp.int32, s.shape, 0)
                cols = lax.broadcasted_iota(jnp.int32, s.shape, 1)
                s = jnp.where(rows >= cols, s, NEG_BIG)
            t = s * c
            m_prev = m_sc[h]
            m_new = jnp.maximum(m_prev, jnp.max(t, axis=1, keepdims=True))
            m_sc[h] = m_new
            p = jnp.exp2(t - jnp.tile(m_new, (1, blk // 128)))
            alpha = jnp.exp2(m_prev - m_new)
            part = p[:, :128]
            for y in range(1, blk // 128):
                part = part + p[:, y * 128:(y + 1) * 128]
            l_sc[h] = l_sc[h] * alpha + part
            acc_sc[h] = acc_sc[h] * jnp.tile(alpha, (1, head // 128)) + dot(p.astype(BF16), v, NN)

    scores(0, s_even)

    @pl.loop(0, i)
    def _(j):
        scores(2 * j + 1, s_odd)
        update(2 * j, s_even, False)
        scores(2 * j + 2, s_even)
        update(2 * j + 1, s_odd, False)

    if z == 0:
        update(2 * i, s_even, True)
    else:
        scores(2 * i + 1, s_odd)
        update(2 * i, s_even, False)
        update(2 * i + 1, s_odd, True)
    for h in range(per):
        total = jnp.sum(l_sc[h], axis=1, keepdims=True)
        o_ref[:, h * head:(h + 1) * head] = (acc_sc[h] / total).astype(BF16)
        lse = m_sc[h] + jnp.log2(jnp.broadcast_to(total, (blk, 128)))
        lse_ref[h:h + 1, :] = lse.T[0:1, :]


def attn_fwd(z, q, k, v, per, head):
    rows = q.shape[0]
    seq = k.shape[0]
    blk = BLK
    pairs = rows * (seq + blk) // 2 * per
    row = pl.BlockSpec((blk, per * head), lambda i: (i, 0))
    whole = pl.BlockSpec((seq, head), lambda i: (0, 0), pipeline_mode=pl.Buffered(1))
    return pl.pallas_call(
        functools.partial(attn_fwd_kernel, z, per, head, blk),
        name='attn_fwd',
        grid=(rows // blk,),
        in_specs=[row, whole, whole],
        out_specs=[row, pl.BlockSpec((per, blk), lambda i: (0, i))],
        out_shape=[jax.ShapeDtypeStruct((rows, per * head), BF16), jax.ShapeDtypeStruct((per, rows), F32)],
        scratch_shapes=[pltpu.VMEM((per, blk, 128), F32), pltpu.VMEM((per, blk, 128), F32), pltpu.VMEM((per, blk, head), F32),
                        pltpu.VMEM((per, blk, blk), F32), pltpu.VMEM((per, blk, blk), F32)],
        compiler_params=pltpu.CompilerParams(dimension_semantics=('arbitrary',), vmem_limit_bytes=VMEM_LIMIT),
        cost_estimate=pl.CostEstimate(flops=4 * pairs * head, bytes_accessed=rows * head * 4 * per + seq * head * 4, transcendentals=pairs),
    )(q, k, v)


def attn_bwd_kernel(z, per, head, blk, q_ref, do_ref, o_ref, lse_ref, k_ref, v_ref, *refs):
    if z == 0:
        dq_ref, dk_ref, dv_ref, dk_acc, dv_acc, dq_acc, q_sc, do_sc, delta_sc, sems = refs
    else:
        dk_in, dv_in, dq_ref, dk_ref, dv_ref, dk_acc, dv_acc, dq_acc, q_sc, do_sc, delta_sc, sems = refs
    i = pl.program_id(0)
    last = pl.num_programs(0) - 1
    scale = head ** -0.5
    c = LOG2E * scale

    @pl.when(i == 0)
    def _():
        if z == 0:
            dk_acc[...] = jnp.zeros_like(dk_acc)
            dv_acc[...] = jnp.zeros_like(dv_acc)
        else:
            loads = [pltpu.make_async_copy(dk_in, dk_acc, sems.at[0]), pltpu.make_async_copy(dv_in, dv_acc, sems.at[1])]
            for load in loads:
                load.start()
            for load in loads:
                load.wait()

    for h in range(per):
        lanes = slice(h * head, (h + 1) * head)
        rows = slice(h * blk, (h + 1) * blk)
        q_sc[rows, :] = q_ref[:, lanes]
        do_sc[rows, :] = do_ref[:, lanes]
        prod = do_ref[:, lanes].astype(F32) * o_ref[:, lanes].astype(F32)
        delta = jnp.broadcast_to(jnp.sum(prod, axis=1, keepdims=True), (blk, 128))
        delta_sc[:, rows] = delta.T[0:1, :]

    def step(j, diag):
        at = pl.ds(pl.multiple_of(j * blk, blk), blk)
        k = k_ref[at, :]
        v = v_ref[at, :]
        dvs = []
        dks = []
        dqs = []
        for h in range(per):
            rows = slice(h * blk, (h + 1) * blk)
            q = q_sc[rows, :]
            d_out = do_sc[rows, :]
            s = dot(k, q, NT)
            p = jnp.exp2(s * c - lse_ref[h:h + 1, :])
            if diag:
                kv_ids = lax.broadcasted_iota(jnp.int32, s.shape, 0)
                q_ids = lax.broadcasted_iota(jnp.int32, s.shape, 1)
                p = jnp.where(q_ids >= kv_ids, p, 0.0)
            dp = dot(v, d_out, NT)
            ds = (p * (dp - delta_sc[:, rows])).astype(BF16)
            dvs.append(dot(p.astype(BF16), d_out, NN))
            dks.append(dot(ds, q, NN))
            dqs.append(dot(ds, k, TN))
        dv_acc[at, :] += functools.reduce(jnp.add, dvs)
        dk_acc[at, :] += functools.reduce(jnp.add, dks)
        for h in range(per):
            rows = slice(h * blk, (h + 1) * blk)
            if diag:
                dq_acc[rows, :] = dqs[h]
            else:
                dq_acc[rows, :] += dqs[h]

    step(2 * i + z, True)

    @pl.loop(0, 2 * i + z)
    def _(j):
        step(j, False)

    for h in range(per):
        dq_ref[:, h * head:(h + 1) * head] = (dq_acc[h * blk:(h + 1) * blk, :] * scale).astype(BF16)

    @pl.when(i == last)
    def _():
        if z == 0:
            stores = [pltpu.make_async_copy(dk_acc, dk_ref, sems.at[0]), pltpu.make_async_copy(dv_acc, dv_ref, sems.at[1])]
            for store in stores:
                store.start()
            for store in stores:
                store.wait()
        else:
            @pl.loop(0, dk_acc.shape[0] // blk)
            def _(j):
                at = pl.ds(pl.multiple_of(j * blk, blk), blk)
                dk_ref[at, :] = (dk_acc[at, :] * scale).astype(BF16)
                dv_ref[at, :] = dv_acc[at, :].astype(BF16)


def attn_bwd(z, q, d_out, o, lse, k, v, per, head, partial):
    rows = q.shape[0]
    seq = k.shape[0]
    blk = BLK
    pairs = rows * (seq + blk) // 2 * per
    row = pl.BlockSpec((blk, per * head), lambda i: (i, 0))
    once = lambda n: pl.BlockSpec((n, head), lambda i: (0, 0), pipeline_mode=pl.Buffered(1))
    anywhere = pl.BlockSpec(memory_space=pl.ANY)
    dq_shape = jax.ShapeDtypeStruct((rows, per * head), BF16)
    if z == 0:
        out_specs = [row, anywhere, anywhere]
        out_shape = [dq_shape, jax.ShapeDtypeStruct((seq, head), F32), jax.ShapeDtypeStruct((seq, head), F32)]
    else:
        out_specs = [row, once(seq), once(seq)]
        out_shape = [dq_shape, jax.ShapeDtypeStruct((seq, head), BF16), jax.ShapeDtypeStruct((seq, head), BF16)]
    return pl.pallas_call(
        functools.partial(attn_bwd_kernel, z, per, head, blk),
        name='attn_bwd',
        grid=(rows // blk,),
        in_specs=[row, row, row, pl.BlockSpec((per, blk), lambda i: (0, i)), once(seq), once(seq)] + [anywhere] * len(partial),
        out_specs=out_specs,
        out_shape=out_shape,
        scratch_shapes=[pltpu.VMEM((seq, head), F32), pltpu.VMEM((seq, head), F32), pltpu.VMEM((per * blk, head), F32),
                        pltpu.VMEM((per * blk, head), BF16), pltpu.VMEM((per * blk, head), BF16), pltpu.VMEM((1, per * blk), F32),
                        pltpu.SemaphoreType.DMA((2,))],
        compiler_params=pltpu.CompilerParams(dimension_semantics=('arbitrary',), vmem_limit_bytes=VMEM_LIMIT),
        cost_estimate=pl.CostEstimate(flops=10 * pairs * head, bytes_accessed=rows * head * 8 * per + seq * head * 16, transcendentals=pairs),
    )(q, d_out, o, lse, k, v, *partial)


def solution(mesh):
    group = mesh.shape['sp']

    def gather(arr, axis=0):
        return lax.all_gather(arr, 'sp', axis=axis, tiled=True)

    def exchange(arr):
        return lax.all_to_all(arr.reshape(group, -1, arr.shape[1]), 'sp', 0, 0, tiled=True)

    def device_step(x_in, dy_in, positions, w_q, w_k, w_v, w_o, w_pre, w_post, q_norm, k_norm):
        _, _, width = x_in.shape
        head = q_norm.shape[0]
        n_q = w_q.shape[1] // head // group
        n_k = w_k.shape[1] // head // group
        per = n_q // n_k
        me = lax.axis_index('sp')
        halves = [slice(z * BLK, (z + 1) * BLK) for z in range(2)]
        dy_half = [dy_in[0, rows] for rows in halves]
        x_half = [x_in[0, rows] for rows in halves]

        def mine(w, n, axis):
            return lax.dynamic_slice_in_dim(w, me * n * head, n * head, axis)

        x_f32, normed, pre_pull, normed_all = [], [], [], []
        for z in range(2):
            if z == 1:
                x_half[1], normed[0] = lax.optimization_barrier((x_half[1], normed[0]))
                normed_all.append(gather(normed[0]))
            x_f32.append(x_half[z].astype(F32))
            out, pull = jax.vjp(pre_norm, x_f32[z], w_pre)
            normed.append(out)
            pre_pull.append(pull)
        normed_all.append(gather(normed[1]))
        cosines, sines = rope_tables(gather(positions), head)
        w_mine = jnp.concatenate([mine(w_q, n_q, 1), mine(w_k, n_k, 1), mine(w_v, n_k, 1)], axis=1)
        qn = q_norm[None, :]
        kn = k_norm[None, :]
        qkv, q_all, kv = [], [], ()
        for z in range(2):
            qkv.append(dot(normed_all[z], w_mine, NN).astype(BF16))
            q, *kv = rope_fwd(z, qkv[z], cosines, sines, qn, kn, n_q, n_k, head, kv)
            q_all.append(q)
        k_all, v_all = kv

        w_o3 = w_o.reshape(group, n_q * head, width)
        o_all, lse, y_out, dy_f32, d_proj_all, dw_post = [], [], [], [], [], []
        for z in range(2):
            o, row_lse = attn_fwd(z, q_all[z], k_all, v_all, per, head)
            o_all.append(o)
            lse.append(row_lse)
        o_mine = [exchange(o) for o in o_all]
        for z in range(2):
            proj = jnp.einsum('gtn,gnd->td', o_mine[z], w_o3, preferred_element_type=F32).astype(BF16)
            post, post_pull = jax.vjp(post_norm, proj, w_post)
            y_out.append((x_f32[z] + post).astype(BF16))
            dy_f32.append(dy_half[z].astype(F32))
            d_proj, dw = post_pull(dy_f32[z])
            dw_post.append(dw)
            if z == 0:
                dy_half[1], d_proj = lax.optimization_barrier((dy_half[1], d_proj))
            d_proj_all.append(gather(d_proj))

        wo_mine = mine(w_o, n_q, 0)
        do_0 = dot(d_proj_all[0], wo_mine, NT).astype(BF16)
        dq_0, *partial = attn_bwd(0, q_all[0], do_0, o_all[0], lse[0], k_all, v_all, per, head, ())
        dq_proj_0, gq_0 = rope_bwd(0, dq_0, (), qkv[0], 0, cosines, sines, qn, n_q, head)
        do_1 = dot(d_proj_all[1], wo_mine, NT).astype(BF16)
        dw_o = (dot(o_all[0], d_proj_all[0], TN) + dot(o_all[1], d_proj_all[1], TN)).astype(BF16)
        do_1, dw_o, dq_proj_0, partial = lax.optimization_barrier((do_1, dw_o, dq_proj_0, partial))
        dw_o = gather(dw_o)
        dq_flat_0 = exchange(dq_proj_0)
        dq_1, dk_all, dv_all = attn_bwd(1, q_all[1], do_1, o_all[1], lse[1], k_all, v_all, per, head, partial)
        dq_1, dk_all, dv_all, dq_flat_0 = lax.optimization_barrier((dq_1, dk_all, dv_all, dq_flat_0))
        dq_proj_1, gq_1 = rope_bwd(1, dq_1, (), qkv[1], 0, cosines, sines, qn, n_q, head)
        dkv, gk = [], []
        for z in range(2):
            out, sums = rope_bwd(z, dk_all, (dv_all,), qkv[z], n_q, cosines, sines, kn, n_k, head)
            dkv.append(out)
            gk.append(sums)
        dq_flat = [dq_flat_0, exchange(dq_proj_1)]
        dq_proj_1, dkv = lax.optimization_barrier((dq_proj_1, dkv))

        def weight_grad(grads):
            return (dot(normed_all[0], grads[0], TN) + dot(normed_all[1], grads[1], TN)).astype(BF16)

        dw_q = weight_grad((dq_proj_0, dq_proj_1))
        dw_q, dw_o, dq_flat[1], dkv = lax.optimization_barrier((dw_q, dw_o, dq_flat[1], dkv))
        dw_q = gather(dw_q, 1)
        dkv_flat = [exchange(dkv[0])]
        dw_kv = weight_grad(dkv)
        dw_kv, dkv_flat[0], dkv[1] = lax.optimization_barrier((dw_kv, dkv_flat[0], dkv[1]))
        dw_k = gather(dw_kv[:, :n_k * head], 1)
        dw_v = gather(dw_kv[:, n_k * head:], 1)
        dkv_flat.append(exchange(dkv[1]))
        dw_o = place(dw_o)

        def back(flat, w):
            return jnp.einsum('gtn,dgn->td', flat, w.reshape(width, group, -1), preferred_element_type=F32)

        dx_out, dw_pre = [], []
        for z in range(2):
            dk_flat = dkv_flat[z][:, :, :n_k * head]
            dv_flat = dkv_flat[z][:, :, n_k * head:]
            d_normed = (back(dq_flat[z], w_q) + back(dk_flat, w_k) + back(dv_flat, w_v)).astype(BF16)
            dx_norm, dw = pre_pull[z](d_normed)
            dw_pre.append(dw)
            dx_out.append((dy_f32[z] + dx_norm).astype(BF16))
        dw_pre = dw_pre[0] + dw_pre[1]
        dw_pre, dw_o = lax.optimization_barrier((dw_pre, dw_o))
        sums = lax.psum((dw_pre, dw_post[0] + dw_post[1], jnp.sum(gq_0 + gq_1, axis=0), jnp.sum(gk[0] + gk[1], axis=0)), 'sp')
        dw_q, sums = lax.optimization_barrier((dw_q, sums))
        return (jnp.concatenate(y_out)[None], jnp.concatenate(dx_out)[None], place(dw_q), place(dw_k), dw_v, dw_o, sums[0], sums[1], sums[2], sums[3])

    token_spec = P('dp', 'sp', None)
    return jax.shard_map(device_step, mesh=mesh,
                         in_specs=(token_spec, token_spec, P(('dp', 'sp')), P(None, None), P(None, None), P(None, None), P(None, None), P(None), P(None), P(None), P(None)),
                         out_specs=(token_spec, token_spec, P('dp', None), P('dp', None), P('dp', None), P('dp', None), P('dp'), P('dp'), P('dp'), P('dp')),
                         check_vma=False)
```

```python
import functools
import jax
import jax.numpy as jnp
from jax import lax
from jax.experimental import pallas as pl
from jax.experimental.pallas import tpu as pltpu
from jax.sharding import PartitionSpec as P

EPS = 1e-6
ROPE_BASE = 1000000.0
ROPE_SCALE = 8.0
NEG_BIG = -1e30
LOG2E = 1.4426950408889634
F32 = jnp.float32
BF16 = jnp.bfloat16
NT = (((1,), (1,)), ((), ()))
NN = (((1,), (0,)), ((), ()))
TN = (((0,), (0,)), ((), ()))
VMEM_LIMIT = 60 * 1024 * 1024


def dot(a, b, dims):
    return lax.dot_general(a, b, dims, preferred_element_type=F32)


def rms_scale(x_f32, weight):
    inv_rms = lax.rsqrt(jnp.mean(x_f32 * x_f32, axis=-1, keepdims=True) + EPS)
    return x_f32 * inv_rms * (1.0 + weight)


def pre_norm(x_f32, weight):
    return rms_scale(x_f32, weight).astype(BF16)


def post_norm(proj, weight):
    return rms_scale(proj.astype(F32), weight)


def rope_tables(positions, head):
    half_dim = head // 2
    inv_freq = ROPE_BASE ** (-jnp.arange(half_dim, dtype=F32) * 2.0 / head)
    angles = (positions.astype(F32) / ROPE_SCALE)[:, None] * inv_freq[None, :]
    return jnp.cos(angles), jnp.sin(angles)


def rope_fwd_kernel(n_q, n_k, head, x_ref, cos_ref, sin_ref, wq_ref, wk_ref, *refs):
    q_ref, k_ref, v_ref = refs[-3:]
    half = head // 2
    cosines = cos_ref[...]
    sines = sin_ref[...]
    for h in range(n_q + n_k):
        x = x_ref[:, h * head:(h + 1) * head].astype(F32)
        w_ref, out_ref, at = (wq_ref, q_ref, h) if h < n_q else (wk_ref, k_ref, h - n_q)
        normed = rms_scale(x, w_ref[...])
        first = normed[:, :half]
        second = normed[:, half:]
        out_ref[:, at * head:at * head + half] = (first * cosines - second * sines).astype(BF16)
        out_ref[:, at * head + half:(at + 1) * head] = (second * cosines + first * sines).astype(BF16)
    v_ref[...] = x_ref[:, (n_q + n_k) * head:]


def rope_fwd(z, qkv, cosines, sines, w_qn, w_kn, n_q, n_k, head, kv_so_far):
    seq = cosines.shape[0]
    blk = BLK
    half = head // 2
    row = lambda width: pl.BlockSpec((blk, width), lambda i: (i, 0))
    placed = lambda width: pl.BlockSpec((blk, width), lambda i: (2 * i + z, 0))
    whole = pl.BlockSpec((1, head), lambda i: (0, 0))
    kv_shape = jax.ShapeDtypeStruct((seq, n_k * head), BF16)
    return pl.pallas_call(
        functools.partial(rope_fwd_kernel, n_q, n_k, head),
        name='rope_fwd',
        grid=(qkv.shape[0] // blk,),
        in_specs=[row((n_q + 2 * n_k) * head), placed(half), placed(half), whole, whole] + [pl.BlockSpec(memory_space=pl.ANY)] * len(kv_so_far),
        out_specs=[row(n_q * head), placed(n_k * head), placed(n_k * head)],
        out_shape=[jax.ShapeDtypeStruct((qkv.shape[0], n_q * head), BF16), kv_shape, kv_shape],
        input_output_aliases={5: 1, 6: 2} if kv_so_far else {},
        compiler_params=pltpu.CompilerParams(dimension_semantics=('arbitrary',)),
        cost_estimate=pl.CostEstimate(flops=qkv.size * 40, bytes_accessed=qkv.size * 4 + seq * head * 2, transcendentals=0),
    )(qkv, cosines, sines, w_qn, w_kn, *kv_so_far)


def rope_bwd_kernel(n, head, d_ref, x_ref, cos_ref, sin_ref, w_ref, *refs):
    out_ref, sum_ref = refs[-2:]
    half = head // 2
    cosines = cos_ref[...]
    sines = sin_ref[...]

    @pl.when(pl.program_id(0) == 0)
    def _():
        sum_ref[...] = jnp.zeros_like(sum_ref)

    for h in range(n):
        x = x_ref[:, h * head:(h + 1) * head].astype(F32)
        d_first = d_ref[:, h * head:h * head + half].astype(F32)
        d_second = d_ref[:, h * head + half:(h + 1) * head].astype(F32)
        g = jnp.concatenate([d_first * cosines + d_second * sines, d_second * cosines - d_first * sines], axis=1)
        inv_rms = lax.rsqrt(jnp.mean(x * x, axis=-1, keepdims=True) + EPS)
        x_hat = x * inv_rms
        sum_ref[...] += jnp.sum((g * x_hat).reshape(x.shape[0] // 8, 8, head), axis=0)
        gw = g * (1.0 + w_ref[...])
        out = inv_rms * (gw - x_hat * jnp.mean(gw * x_hat, axis=-1, keepdims=True))
        out_ref[:, h * head:(h + 1) * head] = out.astype(BF16)
    if len(refs) == 3:
        out_ref[:, n * head:] = refs[0][...]


def rope_bwd(z, grad, beside, qkv, lane_block, cosines, sines, w_n, n, head):
    blk = BLK
    half = head // 2
    row = lambda width: pl.BlockSpec((blk, width), lambda i: (i, 0))
    placed = lambda width: pl.BlockSpec((blk, width), lambda i: (2 * i + z, 0))
    rows = qkv.shape[0]
    lanes = n * head + sum(b.shape[1] for b in beside)
    return pl.pallas_call(
        functools.partial(rope_bwd_kernel, n, head),
        name='rope_bwd',
        grid=(rows // blk,),
        in_specs=[placed(n * head) if beside else row(n * head), pl.BlockSpec((blk, n * head), lambda i: (i, lane_block)),
                  placed(half), placed(half), pl.BlockSpec((1, head), lambda i: (0, 0))] + [placed(b.shape[1]) for b in beside],
        out_specs=[row(lanes), pl.BlockSpec((8, head), lambda i: (0, 0))],
        out_shape=[jax.ShapeDtypeStruct((rows, lanes), BF16), jax.ShapeDtypeStruct((8, head), F32)],
        compiler_params=pltpu.CompilerParams(dimension_semantics=('arbitrary',)),
        cost_estimate=pl.CostEstimate(flops=rows * n * head * 60, bytes_accessed=rows * n * head * 6 + rows * head * 4, transcendentals=0),
    )(grad, qkv, cosines, sines, w_n, *beside)


def copy_kernel(x_ref, o_ref):
    o_ref[...] = x_ref[...]


def place(x):
    rows = 256
    spec = pl.BlockSpec((rows, x.shape[1]), lambda i: (i, 0))
    return pl.pallas_call(
        copy_kernel,
        name='place',
        grid=(x.shape[0] // rows,),
        in_specs=[spec],
        out_specs=spec,
        out_shape=jax.ShapeDtypeStruct(x.shape, x.dtype),
        compiler_params=pltpu.CompilerParams(dimension_semantics=('arbitrary',)),
        cost_estimate=pl.CostEstimate(flops=x.size * 16, bytes_accessed=4 * x.size, transcendentals=0),
    )(x)


BLK = 512


def attn_fwd_kernel(z, per, head, blk, q_ref, k_ref, v_ref, o_ref, lse_ref, m_sc, l_sc, acc_sc, s_even, s_odd):
    i = pl.program_id(0)
    c = LOG2E * head ** -0.5
    m_sc[...] = jnp.full_like(m_sc, -jnp.inf)
    l_sc[...] = jnp.zeros_like(l_sc)
    acc_sc[...] = jnp.zeros_like(acc_sc)

    def scores(j, s_ref):
        k = k_ref[pl.ds(pl.multiple_of(j * blk, blk), blk), :]
        for h in range(per):
            s_ref[h] = dot(q_ref[:, h * head:(h + 1) * head], k, NT)

    def update(j, s_ref, masked):
        v = v_ref[pl.ds(pl.multiple_of(j * blk, blk), blk), :]
        for h in range(per):
            s = s_ref[h]
            if masked:
                rows = lax.broadcasted_iota(jnp.int32, s.shape, 0)
                cols = lax.broadcasted_iota(jnp.int32, s.shape, 1)
                s = jnp.where(rows >= cols, s, NEG_BIG)
            t = s * c
            m_prev = m_sc[h]
            m_new = jnp.maximum(m_prev, jnp.max(t, axis=1, keepdims=True))
            m_sc[h] = m_new
            p = jnp.exp2(t - jnp.tile(m_new, (1, blk // 128)))
            alpha = jnp.exp2(m_prev - m_new)
            part = p[:, :128]
            for y in range(1, blk // 128):
                part = part + p[:, y * 128:(y + 1) * 128]
            l_sc[h] = l_sc[h] * alpha + part
            acc_sc[h] = acc_sc[h] * jnp.tile(alpha, (1, head // 128)) + dot(p.astype(BF16), v, NN)

    scores(0, s_even)

    @pl.loop(0, i)
    def _(j):
        scores(2 * j + 1, s_odd)
        update(2 * j, s_even, False)
        scores(2 * j + 2, s_even)
        update(2 * j + 1, s_odd, False)

    if z == 0:
        update(2 * i, s_even, True)
    else:
        scores(2 * i + 1, s_odd)
        update(2 * i, s_even, False)
        update(2 * i + 1, s_odd, True)
    for h in range(per):
        total = jnp.sum(l_sc[h], axis=1, keepdims=True)
        o_ref[:, h * head:(h + 1) * head] = (acc_sc[h] / total).astype(BF16)
        lse = m_sc[h] + jnp.log2(jnp.broadcast_to(total, (blk, 128)))
        lse_ref[h:h + 1, :] = lse.T[0:1, :]


def attn_fwd(z, q, k, v, per, head):
    rows = q.shape[0]
    seq = k.shape[0]
    blk = BLK
    pairs = rows * (seq + blk) // 2 * per
    row = pl.BlockSpec((blk, per * head), lambda i: (i, 0))
    whole = pl.BlockSpec((seq, head), lambda i: (0, 0), pipeline_mode=pl.Buffered(1))
    return pl.pallas_call(
        functools.partial(attn_fwd_kernel, z, per, head, blk),
        name='attn_fwd',
        grid=(rows // blk,),
        in_specs=[row, whole, whole],
        out_specs=[row, pl.BlockSpec((per, blk), lambda i: (0, i))],
        out_shape=[jax.ShapeDtypeStruct((rows, per * head), BF16), jax.ShapeDtypeStruct((per, rows), F32)],
        scratch_shapes=[pltpu.VMEM((per, blk, 128), F32), pltpu.VMEM((per, blk, 128), F32), pltpu.VMEM((per, blk, head), F32),
                        pltpu.VMEM((per, blk, blk), F32), pltpu.VMEM((per, blk, blk), F32)],
        compiler_params=pltpu.CompilerParams(dimension_semantics=('arbitrary',), vmem_limit_bytes=VMEM_LIMIT),
        cost_estimate=pl.CostEstimate(flops=4 * pairs * head, bytes_accessed=rows * head * 4 * per + seq * head * 4, transcendentals=pairs),
    )(q, k, v)


def attn_bwd_kernel(z, per, head, blk, q_ref, do_ref, o_ref, lse_ref, k_ref, v_ref, *refs):
    if z == 0:
        dq_ref, dk_ref, dv_ref, dk_acc, dv_acc, dq_acc, q_sc, do_sc, delta_sc, sems = refs
    else:
        dk_in, dv_in, dq_ref, dk_ref, dv_ref, dk_acc, dv_acc, dq_acc, q_sc, do_sc, delta_sc, sems = refs
    i = pl.program_id(0)
    last = pl.num_programs(0) - 1
    scale = head ** -0.5
    c = LOG2E * scale

    @pl.when(i == 0)
    def _():
        if z == 0:
            dk_acc[...] = jnp.zeros_like(dk_acc)
            dv_acc[...] = jnp.zeros_like(dv_acc)
        else:
            loads = [pltpu.make_async_copy(dk_in, dk_acc, sems.at[0]), pltpu.make_async_copy(dv_in, dv_acc, sems.at[1])]
            for load in loads:
                load.start()
            for load in loads:
                load.wait()

    for h in range(per):
        lanes = slice(h * head, (h + 1) * head)
        rows = slice(h * blk, (h + 1) * blk)
        q_sc[rows, :] = q_ref[:, lanes]
        do_sc[rows, :] = do_ref[:, lanes]
        prod = do_ref[:, lanes].astype(F32) * o_ref[:, lanes].astype(F32)
        delta = jnp.broadcast_to(jnp.sum(prod, axis=1, keepdims=True), (blk, 128))
        delta_sc[:, rows] = delta.T[0:1, :]

    def step(j, diag):
        at = pl.ds(pl.multiple_of(j * blk, blk), blk)
        k = k_ref[at, :]
        v = v_ref[at, :]
        dvs = []
        dks = []
        dqs = []
        for h in range(per):
            rows = slice(h * blk, (h + 1) * blk)
            q = q_sc[rows, :]
            d_out = do_sc[rows, :]
            s = dot(k, q, NT)
            p = jnp.exp2(s * c - lse_ref[h:h + 1, :])
            if diag:
                kv_ids = lax.broadcasted_iota(jnp.int32, s.shape, 0)
                q_ids = lax.broadcasted_iota(jnp.int32, s.shape, 1)
                p = jnp.where(q_ids >= kv_ids, p, 0.0)
            dp = dot(v, d_out, NT)
            ds = (p * (dp - delta_sc[:, rows])).astype(BF16)
            dvs.append(dot(p.astype(BF16), d_out, NN))
            dks.append(dot(ds, q, NN))
            dqs.append(dot(ds, k, TN))
        dv_acc[at, :] += functools.reduce(jnp.add, dvs)
        dk_acc[at, :] += functools.reduce(jnp.add, dks)
        for h in range(per):
            rows = slice(h * blk, (h + 1) * blk)
            if diag:
                dq_acc[rows, :] = dqs[h]
            else:
                dq_acc[rows, :] += dqs[h]

    step(2 * i + z, True)

    @pl.loop(0, 2 * i + z)
    def _(j):
        step(j, False)

    for h in range(per):
        dq_ref[:, h * head:(h + 1) * head] = (dq_acc[h * blk:(h + 1) * blk, :] * scale).astype(BF16)

    @pl.when(i == last)
    def _():
        if z == 0:
            stores = [pltpu.make_async_copy(dk_acc, dk_ref, sems.at[0]), pltpu.make_async_copy(dv_acc, dv_ref, sems.at[1])]
            for store in stores:
                store.start()
            for store in stores:
                store.wait()
        else:
            @pl.loop(0, dk_acc.shape[0] // blk)
            def _(j):
                at = pl.ds(pl.multiple_of(j * blk, blk), blk)
                dk_ref[at, :] = (dk_acc[at, :] * scale).astype(BF16)
                dv_ref[at, :] = dv_acc[at, :].astype(BF16)


def attn_bwd(z, q, d_out, o, lse, k, v, per, head, partial):
    rows = q.shape[0]
    seq = k.shape[0]
    blk = BLK
    pairs = rows * (seq + blk) // 2 * per
    row = pl.BlockSpec((blk, per * head), lambda i: (i, 0))
    once = lambda n: pl.BlockSpec((n, head), lambda i: (0, 0), pipeline_mode=pl.Buffered(1))
    anywhere = pl.BlockSpec(memory_space=pl.ANY)
    dq_shape = jax.ShapeDtypeStruct((rows, per * head), BF16)
    if z == 0:
        out_specs = [row, anywhere, anywhere]
        out_shape = [dq_shape, jax.ShapeDtypeStruct((seq, head), F32), jax.ShapeDtypeStruct((seq, head), F32)]
    else:
        out_specs = [row, once(seq), once(seq)]
        out_shape = [dq_shape, jax.ShapeDtypeStruct((seq, head), BF16), jax.ShapeDtypeStruct((seq, head), BF16)]
    return pl.pallas_call(
        functools.partial(attn_bwd_kernel, z, per, head, blk),
        name='attn_bwd',
        grid=(rows // blk,),
        in_specs=[row, row, row, pl.BlockSpec((per, blk), lambda i: (0, i)), once(seq), once(seq)] + [anywhere] * len(partial),
        out_specs=out_specs,
        out_shape=out_shape,
        scratch_shapes=[pltpu.VMEM((seq, head), F32), pltpu.VMEM((seq, head), F32), pltpu.VMEM((per * blk, head), F32),
                        pltpu.VMEM((per * blk, head), BF16), pltpu.VMEM((per * blk, head), BF16), pltpu.VMEM((1, per * blk), F32),
                        pltpu.SemaphoreType.DMA((2,))],
        compiler_params=pltpu.CompilerParams(dimension_semantics=('arbitrary',), vmem_limit_bytes=VMEM_LIMIT),
        cost_estimate=pl.CostEstimate(flops=10 * pairs * head, bytes_accessed=rows * head * 8 * per + seq * head * 16, transcendentals=pairs),
    )(q, d_out, o, lse, k, v, *partial)


def solution(mesh):
    group = mesh.shape['sp']

    def gather(arr, axis=0):
        return lax.all_gather(arr, 'sp', axis=axis, tiled=True)

    def exchange(arr):
        return lax.all_to_all(arr.reshape(group, -1, arr.shape[1]), 'sp', 0, 0, tiled=True)

    def device_step(x_in, dy_in, positions, w_q, w_k, w_v, w_o, w_pre, w_post, q_norm, k_norm):
        _, _, width = x_in.shape
        head = q_norm.shape[0]
        n_q = w_q.shape[1] // head // group
        n_k = w_k.shape[1] // head // group
        per = n_q // n_k
        me = lax.axis_index('sp')
        halves = [slice(z * BLK, (z + 1) * BLK) for z in range(2)]
        dy_half = [dy_in[0, rows] for rows in halves]
        x_half = [x_in[0, rows] for rows in halves]

        def mine(w, n, axis):
            return lax.dynamic_slice_in_dim(w, me * n * head, n * head, axis)

        x_f32, normed, pre_pull, normed_all = [], [], [], []
        for z in range(2):
            if z == 1:
                x_half[1], normed[0] = lax.optimization_barrier((x_half[1], normed[0]))
                normed_all.append(gather(normed[0]))
            x_f32.append(x_half[z].astype(F32))
            out, pull = jax.vjp(pre_norm, x_f32[z], w_pre)
            normed.append(out)
            pre_pull.append(pull)
        cosines, sines = rope_tables(gather(positions), head)
        w_mine = jnp.concatenate([mine(w_q, n_q, 1), mine(w_k, n_k, 1), mine(w_v, n_k, 1)], axis=1)
        qn = q_norm[None, :]
        kn = k_norm[None, :]
        local = [dot(normed[1], w, NN).astype(BF16).reshape(BLK, group, -1) for w in (w_k, w_v, w_q)]
        local = jnp.concatenate([local[2], local[0], local[1]], axis=2).swapaxes(0, 1)
        local = lax.all_to_all(local, 'sp', 0, 0, tiled=True)
        qkv = [dot(normed_all[0], w_mine, NN).astype(BF16), local.reshape(group * BLK, -1)]
        q_all, kv = [], ()
        for z in range(2):
            q, *kv = rope_fwd(z, qkv[z], cosines, sines, qn, kn, n_q, n_k, head, kv)
            q_all.append(q)
        k_all, v_all, to_gather = lax.optimization_barrier((*kv, normed[1]))
        normed_all.append(gather(to_gather))

        w_o3 = w_o.reshape(group, n_q * head, width)
        o_all, lse, y_out, dy_f32, d_proj_all, dw_post = [], [], [], [], [], []
        for z in range(2):
            o, row_lse = attn_fwd(z, q_all[z], k_all, v_all, per, head)
            o_all.append(o)
            lse.append(row_lse)
        o_mine = [exchange(o_all[0])]
        o_mine[0], o_all[1] = lax.optimization_barrier((o_mine[0], o_all[1]))
        o_mine.append(exchange(o_all[1]))
        for z in range(2):
            proj = jnp.einsum('gtn,gnd->td', o_mine[z], w_o3, preferred_element_type=F32).astype(BF16)
            post, post_pull = jax.vjp(post_norm, proj, w_post)
            y_out.append((x_f32[z] + post).astype(BF16))
            dy_f32.append(dy_half[z].astype(F32))
            d_proj, dw = post_pull(dy_f32[z])
            dw_post.append(dw)
            if z == 0:
                dy_half[1], d_proj, o_mine[1], normed_all[1] = lax.optimization_barrier((dy_half[1], d_proj, o_mine[1], normed_all[1]))
            d_proj_all.append(gather(d_proj))

        wo_mine = mine(w_o, n_q, 0)
        do_0 = dot(d_proj_all[0], wo_mine, NT).astype(BF16)
        dq_0, *partial = attn_bwd(0, q_all[0], do_0, o_all[0], lse[0], k_all, v_all, per, head, ())
        dq_proj_0, gq_0 = rope_bwd(0, dq_0, (), qkv[0], 0, cosines, sines, qn, n_q, head)
        do_1 = dot(d_proj_all[1], wo_mine, NT).astype(BF16)
        dw_o = (dot(o_all[0], d_proj_all[0], TN) + dot(o_all[1], d_proj_all[1], TN)).astype(BF16)
        dq_flat_0 = exchange(dq_proj_0)
        do_1, dw_o, dq_flat_0, partial = lax.optimization_barrier((do_1, dw_o, dq_flat_0, partial))
        dw_o = gather(dw_o)
        dq_1, dk_all, dv_all = attn_bwd(1, q_all[1], do_1, o_all[1], lse[1], k_all, v_all, per, head, partial)
        dq_proj_1, gq_1 = rope_bwd(1, dq_1, (), qkv[1], 0, cosines, sines, qn, n_q, head)
        dq_flat = [dq_flat_0, exchange(dq_proj_1)]

        def weight_grad(grads):
            return (dot(normed_all[0], grads[0], TN) + dot(normed_all[1], grads[1], TN)).astype(BF16)

        dw_q = weight_grad((dq_proj_0, dq_proj_1))
        dw_q, dw_o, dq_flat[1], dk_all, dv_all = lax.optimization_barrier((dw_q, dw_o, dq_flat[1], dk_all, dv_all))
        dw_q = gather(dw_q, 1)
        dkv, gk = [], []
        for z in range(2):
            out, sums = rope_bwd(z, dk_all, (dv_all,), qkv[z], n_q, cosines, sines, kn, n_k, head)
            dkv.append(out)
            gk.append(sums)
        dkv_flat = [exchange(dkv[0])]
        dw_kv = weight_grad(dkv)
        dw_kv, dkv_flat[0], dkv[1] = lax.optimization_barrier((dw_kv, dkv_flat[0], dkv[1]))
        dw_k = gather(dw_kv[:, :n_k * head], 1)
        dw_v = gather(dw_kv[:, n_k * head:], 1)
        dkv_flat.append(exchange(dkv[1]))
        dw_o = place(dw_o)

        def back(flat, w):
            return jnp.einsum('gtn,dgn->td', flat, w.reshape(width, group, -1), preferred_element_type=F32)

        dx_out, dw_pre = [], []
        for z in range(2):
            dk_flat = dkv_flat[z][:, :, :n_k * head]
            dv_flat = dkv_flat[z][:, :, n_k * head:]
            d_normed = (back(dq_flat[z], w_q) + back(dk_flat, w_k) + back(dv_flat, w_v)).astype(BF16)
            dx_norm, dw = pre_pull[z](d_normed)
            dw_pre.append(dw)
            dx_out.append((dy_f32[z] + dx_norm).astype(BF16))
        dw_pre = dw_pre[0] + dw_pre[1]
        dw_pre, dw_o = lax.optimization_barrier((dw_pre, dw_o))
        sums = lax.psum((dw_pre, dw_post[0] + dw_post[1], jnp.sum(gq_0 + gq_1, axis=0), jnp.sum(gk[0] + gk[1], axis=0)), 'sp')
        dw_q, sums = lax.optimization_barrier((dw_q, sums))
        return (jnp.concatenate(y_out)[None], jnp.concatenate(dx_out)[None], place(dw_q), place(dw_k), dw_v, dw_o, sums[0], sums[1], sums[2], sums[3])

    token_spec = P('dp', 'sp', None)
    return jax.shard_map(device_step, mesh=mesh,
                         in_specs=(token_spec, token_spec, P(('dp', 'sp')), P(None, None), P(None, None), P(None, None), P(None, None), P(None), P(None), P(None), P(None)),
                         out_specs=(token_spec, token_spec, P('dp', None), P('dp', None), P('dp', None), P('dp', None), P('dp'), P('dp'), P('dp'), P('dp')),
                         check_vma=False)
```

```python
import functools
import jax
import jax.numpy as jnp
from jax import lax
from jax.experimental import pallas as pl
from jax.experimental.pallas import tpu as pltpu
from jax.sharding import PartitionSpec as P

EPS = 1e-6
ROPE_BASE = 1000000.0
ROPE_SCALE = 8.0
NEG_BIG = -1e30
LOG2E = 1.4426950408889634
F32 = jnp.float32
BF16 = jnp.bfloat16
NT = (((1,), (1,)), ((), ()))
NN = (((1,), (0,)), ((), ()))
TN = (((0,), (0,)), ((), ()))
VMEM_LIMIT = 60 * 1024 * 1024


def dot(a, b, dims):
    return lax.dot_general(a, b, dims, preferred_element_type=F32)


def rms_scale(x_f32, weight):
    inv_rms = lax.rsqrt(jnp.mean(x_f32 * x_f32, axis=-1, keepdims=True) + EPS)
    return x_f32 * inv_rms * (1.0 + weight)


def pre_norm(x_f32, weight):
    return rms_scale(x_f32, weight).astype(BF16)


def post_norm(proj, weight):
    return rms_scale(proj.astype(F32), weight)


def rope_tables(positions, head):
    half_dim = head // 2
    inv_freq = ROPE_BASE ** (-jnp.arange(half_dim, dtype=F32) * 2.0 / head)
    angles = (positions.astype(F32) / ROPE_SCALE)[:, None] * inv_freq[None, :]
    return jnp.cos(angles), jnp.sin(angles)


def rope_fwd_kernel(n_q, n_k, head, x_ref, cos_ref, sin_ref, wq_ref, wk_ref, *refs):
    q_ref, k_ref, v_ref, kt_ref, vt_ref = refs[-5:]
    half = head // 2
    cosines = cos_ref[...]
    sines = sin_ref[...]
    for h in range(n_q + n_k):
        x = x_ref[:, h * head:(h + 1) * head].astype(F32)
        w_ref, out_ref, at = (wq_ref, q_ref, h) if h < n_q else (wk_ref, k_ref, h - n_q)
        normed = rms_scale(x, w_ref[...])
        first = normed[:, :half]
        second = normed[:, half:]
        out_ref[:, at * head:at * head + half] = (first * cosines - second * sines).astype(BF16)
        out_ref[:, at * head + half:(at + 1) * head] = (second * cosines + first * sines).astype(BF16)
    v_ref[...] = x_ref[:, (n_q + n_k) * head:]
    kt_ref[...] = k_ref[...].T
    vt_ref[...] = v_ref[...].T


def rope_fwd(z, qkv, cosines, sines, w_qn, w_kn, n_q, n_k, head, kv_so_far):
    seq = cosines.shape[0]
    blk = BLK
    half = head // 2
    row = lambda width: pl.BlockSpec((blk, width), lambda i: (i, 0))
    placed = lambda width: pl.BlockSpec((blk, width), lambda i: (2 * i + z, 0))
    whole = pl.BlockSpec((1, head), lambda i: (0, 0))
    kv_shape = jax.ShapeDtypeStruct((seq, n_k * head), BF16)
    t_shape = jax.ShapeDtypeStruct((n_k * head, seq), BF16)
    t_placed = pl.BlockSpec((n_k * head, blk), lambda i: (0, 2 * i + z))
    return pl.pallas_call(
        functools.partial(rope_fwd_kernel, n_q, n_k, head),
        name='rope_fwd',
        grid=(qkv.shape[0] // blk,),
        in_specs=[row((n_q + 2 * n_k) * head), placed(half), placed(half), whole, whole] + [pl.BlockSpec(memory_space=pl.ANY)] * len(kv_so_far),
        out_specs=[row(n_q * head), placed(n_k * head), placed(n_k * head), t_placed, t_placed],
        out_shape=[jax.ShapeDtypeStruct((qkv.shape[0], n_q * head), BF16), kv_shape, kv_shape, t_shape, t_shape],
        input_output_aliases={5: 1, 6: 2, 7: 3, 8: 4} if kv_so_far else {},
        compiler_params=pltpu.CompilerParams(dimension_semantics=('arbitrary',)),
        cost_estimate=pl.CostEstimate(flops=qkv.size * 40, bytes_accessed=qkv.size * 4 + seq * head * 2, transcendentals=0),
    )(qkv, cosines, sines, w_qn, w_kn, *kv_so_far)


def rope_bwd_kernel(n, head, d_ref, x_ref, cos_ref, sin_ref, w_ref, *refs):
    out_ref, sum_ref = refs[-2:]
    half = head // 2
    cosines = cos_ref[...]
    sines = sin_ref[...]

    @pl.when(pl.program_id(0) == 0)
    def _():
        sum_ref[...] = jnp.zeros_like(sum_ref)

    for h in range(n):
        x = x_ref[:, h * head:(h + 1) * head].astype(F32)
        d_first = d_ref[:, h * head:h * head + half].astype(F32)
        d_second = d_ref[:, h * head + half:(h + 1) * head].astype(F32)
        g = jnp.concatenate([d_first * cosines + d_second * sines, d_second * cosines - d_first * sines], axis=1)
        inv_rms = lax.rsqrt(jnp.mean(x * x, axis=-1, keepdims=True) + EPS)
        x_hat = x * inv_rms
        sum_ref[...] += jnp.sum((g * x_hat).reshape(x.shape[0] // 8, 8, head), axis=0)
        gw = g * (1.0 + w_ref[...])
        out = inv_rms * (gw - x_hat * jnp.mean(gw * x_hat, axis=-1, keepdims=True))
        out_ref[:, h * head:(h + 1) * head] = out.astype(BF16)
    if len(refs) == 3:
        out_ref[:, n * head:] = refs[0][...]


def rope_bwd(z, grad, beside, qkv, lane_block, cosines, sines, w_n, n, head):
    blk = BLK
    half = head // 2
    row = lambda width: pl.BlockSpec((blk, width), lambda i: (i, 0))
    placed = lambda width: pl.BlockSpec((blk, width), lambda i: (2 * i + z, 0))
    rows = qkv.shape[0]
    lanes = n * head + sum(b.shape[1] for b in beside)
    return pl.pallas_call(
        functools.partial(rope_bwd_kernel, n, head),
        name='rope_bwd',
        grid=(rows // blk,),
        in_specs=[placed(n * head) if beside else row(n * head), pl.BlockSpec((blk, n * head), lambda i: (i, lane_block)),
                  placed(half), placed(half), pl.BlockSpec((1, head), lambda i: (0, 0))] + [placed(b.shape[1]) for b in beside],
        out_specs=[row(lanes), pl.BlockSpec((8, head), lambda i: (0, 0))],
        out_shape=[jax.ShapeDtypeStruct((rows, lanes), BF16), jax.ShapeDtypeStruct((8, head), F32)],
        compiler_params=pltpu.CompilerParams(dimension_semantics=('arbitrary',)),
        cost_estimate=pl.CostEstimate(flops=rows * n * head * 60, bytes_accessed=rows * n * head * 6 + rows * head * 4, transcendentals=0),
    )(grad, qkv, cosines, sines, w_n, *beside)


def copy_kernel(x_ref, o_ref):
    o_ref[...] = x_ref[...]


def place(x):
    rows = 256
    spec = pl.BlockSpec((rows, x.shape[1]), lambda i: (i, 0))
    return pl.pallas_call(
        copy_kernel,
        name='place',
        grid=(x.shape[0] // rows,),
        in_specs=[spec],
        out_specs=spec,
        out_shape=jax.ShapeDtypeStruct(x.shape, x.dtype),
        compiler_params=pltpu.CompilerParams(dimension_semantics=('arbitrary',)),
        cost_estimate=pl.CostEstimate(flops=x.size * 16, bytes_accessed=4 * x.size, transcendentals=0),
    )(x)


def split_kernel(x_ref, *refs):
    a_ref, b_ref = refs[-2:]
    a_ref[...] = x_ref[:, :a_ref.shape[1]]
    b_ref[...] = x_ref[:, a_ref.shape[1]:]


def split_pairs(x, lanes, out_rows, first_row, so_far):
    rows = x.shape[0] // 3
    parts = x.shape[1] // (2 * lanes)
    out = pl.BlockSpec((rows, lanes), lambda i, g: (i + first_row // rows, g))
    shape = jax.ShapeDtypeStruct((out_rows, parts * lanes), x.dtype)
    return pl.pallas_call(
        split_kernel,
        name='split_pairs',
        grid=(3, parts),
        in_specs=[pl.BlockSpec((rows, 2 * lanes), lambda i, g: (i, g))] + [pl.BlockSpec(memory_space=pl.ANY)] * len(so_far),
        out_specs=[out, out],
        out_shape=[shape, shape],
        input_output_aliases={1: 0, 2: 1} if so_far else {},
        compiler_params=pltpu.CompilerParams(dimension_semantics=('arbitrary', 'arbitrary')),
        cost_estimate=pl.CostEstimate(flops=x.size * 16, bytes_accessed=4 * x.size, transcendentals=0),
    )(x, *so_far)


BLK = 512


def attn_fwd_kernel(z, per, head, blk, q_ref, k_ref, vt_ref, o_ref, lse_ref, m_sc, l_sc, acc_sc, s_even, s_odd):
    i = pl.program_id(0)
    c = LOG2E * head ** -0.5
    m_sc[...] = jnp.full_like(m_sc, -jnp.inf)
    l_sc[...] = jnp.zeros_like(l_sc)
    acc_sc[...] = jnp.zeros_like(acc_sc)

    def scores(j, s_ref):
        k = k_ref[pl.ds(pl.multiple_of(j * blk, blk), blk), :]
        for h in range(per):
            s_ref[h] = dot(k, q_ref[:, h * head:(h + 1) * head], NT)

    def update(j, s_ref, masked):
        v_t = vt_ref[:, pl.ds(pl.multiple_of(j * blk, blk), blk)]
        for h in range(per):
            s = s_ref[h]
            if masked:
                kv_ids = lax.broadcasted_iota(jnp.int32, s.shape, 0)
                q_ids = lax.broadcasted_iota(jnp.int32, s.shape, 1)
                s = jnp.where(q_ids >= kv_ids, s, NEG_BIG)
            t = s * c
            m_prev = m_sc[h]
            m_new = jnp.maximum(m_prev, jnp.max(t, axis=0, keepdims=True))
            m_sc[h] = m_new
            p = jnp.exp2(t - m_new)
            alpha = jnp.exp2(m_prev - m_new)
            l_sc[h] = l_sc[h] * alpha + jnp.sum(p.reshape(blk // 8, 8, blk), axis=0)
            acc_sc[h] = acc_sc[h] * alpha + dot(v_t, p.astype(BF16), NN)

    scores(0, s_even)

    @pl.loop(0, i)
    def _(j):
        scores(2 * j + 1, s_odd)
        update(2 * j, s_even, False)
        scores(2 * j + 2, s_even)
        update(2 * j + 1, s_odd, False)

    if z == 0:
        update(2 * i, s_even, True)
    else:
        scores(2 * i + 1, s_odd)
        update(2 * i, s_even, False)
        update(2 * i + 1, s_odd, True)
    for h in range(per):
        total = jnp.sum(l_sc[h], axis=0, keepdims=True)
        o_ref[:, h * head:(h + 1) * head] = (acc_sc[h] / total).T.astype(BF16)
        lse_ref[h:h + 1, :] = m_sc[h] + jnp.log2(total)


def attn_fwd(z, q, k, v_t, per, head):
    rows = q.shape[0]
    seq = k.shape[0]
    blk = BLK
    pairs = rows * (seq + blk) // 2 * per
    row = pl.BlockSpec((blk, per * head), lambda i: (i, 0))
    whole = pl.BlockSpec((seq, head), lambda i: (0, 0), pipeline_mode=pl.Buffered(1))
    return pl.pallas_call(
        functools.partial(attn_fwd_kernel, z, per, head, blk),
        name='attn_fwd',
        grid=(rows // blk,),
        in_specs=[row, whole, pl.BlockSpec((head, seq), lambda i: (0, 0), pipeline_mode=pl.Buffered(1))],
        out_specs=[row, pl.BlockSpec((per, blk), lambda i: (0, i))],
        out_shape=[jax.ShapeDtypeStruct((rows, per * head), BF16), jax.ShapeDtypeStruct((per, rows), F32)],
        scratch_shapes=[pltpu.VMEM((per, 1, blk), F32), pltpu.VMEM((per, 8, blk), F32), pltpu.VMEM((per, head, blk), F32),
                        pltpu.VMEM((per, blk, blk), F32), pltpu.VMEM((per, blk, blk), F32)],
        compiler_params=pltpu.CompilerParams(dimension_semantics=('arbitrary',), vmem_limit_bytes=VMEM_LIMIT),
        cost_estimate=pl.CostEstimate(flops=4 * pairs * head, bytes_accessed=rows * head * 4 * per + seq * head * 4, transcendentals=pairs),
    )(q, k, v_t)


def attn_bwd_kernel(z, per, head, blk, q_ref, do_ref, o_ref, lse_ref, k_ref, v_ref, kt_ref, *refs):
    if z == 0:
        dq_ref, dk_ref, dv_ref, dk_acc, dv_acc, dq_acc, q_sc, do_sc, delta_sc, sems = refs
    else:
        dk_in, dv_in, dq_ref, dk_ref, dv_ref, dk_acc, dv_acc, dq_acc, q_sc, do_sc, delta_sc, sems = refs
    i = pl.program_id(0)
    last = pl.num_programs(0) - 1
    scale = head ** -0.5
    c = LOG2E * scale

    @pl.when(i == 0)
    def _():
        if z == 0:
            dk_acc[...] = jnp.zeros_like(dk_acc)
            dv_acc[...] = jnp.zeros_like(dv_acc)
        else:
            loads = [pltpu.make_async_copy(dk_in, dk_acc, sems.at[0]), pltpu.make_async_copy(dv_in, dv_acc, sems.at[1])]
            for load in loads:
                load.start()
            for load in loads:
                load.wait()

    for h in range(per):
        lanes = slice(h * head, (h + 1) * head)
        rows = slice(h * blk, (h + 1) * blk)
        q_sc[rows, :] = q_ref[:, lanes]
        do_sc[rows, :] = do_ref[:, lanes]
        prod = do_ref[:, lanes].astype(F32) * o_ref[:, lanes].astype(F32)
        delta = jnp.broadcast_to(jnp.sum(prod, axis=1, keepdims=True), (blk, 128))
        delta_sc[:, rows] = delta.T[0:1, :]

    def step(j, diag):
        at = pl.ds(pl.multiple_of(j * blk, blk), blk)
        k = k_ref[at, :]
        v = v_ref[at, :]
        k_t = kt_ref[:, at]
        dvs = []
        dks = []
        dqs = []
        for h in range(per):
            rows = slice(h * blk, (h + 1) * blk)
            q = q_sc[rows, :]
            d_out = do_sc[rows, :]
            s = dot(k, q, NT)
            p = jnp.exp2(s * c - lse_ref[h:h + 1, :])
            if diag:
                kv_ids = lax.broadcasted_iota(jnp.int32, s.shape, 0)
                q_ids = lax.broadcasted_iota(jnp.int32, s.shape, 1)
                p = jnp.where(q_ids >= kv_ids, p, 0.0)
            dp = dot(v, d_out, NT)
            ds = (p * (dp - delta_sc[:, rows])).astype(BF16)
            dvs.append(dot(p.astype(BF16), d_out, NN))
            dks.append(dot(ds, q, NN))
            dqs.append(dot(k_t, ds, NN))
        dv_acc[at, :] += functools.reduce(jnp.add, dvs)
        dk_acc[at, :] += functools.reduce(jnp.add, dks)
        for h in range(per):
            if diag:
                dq_acc[h] = dqs[h]
            else:
                dq_acc[h] += dqs[h]

    step(2 * i + z, True)

    @pl.loop(0, 2 * i + z)
    def _(j):
        step(j, False)

    for h in range(per):
        dq_ref[:, h * head:(h + 1) * head] = (dq_acc[h] * scale).T.astype(BF16)

    @pl.when(i == last)
    def _():
        if z == 0:
            stores = [pltpu.make_async_copy(dk_acc, dk_ref, sems.at[0]), pltpu.make_async_copy(dv_acc, dv_ref, sems.at[1])]
            for store in stores:
                store.start()
            for store in stores:
                store.wait()
        else:
            @pl.loop(0, dk_acc.shape[0] // blk)
            def _(j):
                at = pl.ds(pl.multiple_of(j * blk, blk), blk)
                dk_ref[at, :] = (dk_acc[at, :] * scale).astype(BF16)
                dv_ref[at, :] = dv_acc[at, :].astype(BF16)


def attn_bwd(z, q, d_out, o, lse, k, v, k_t, per, head, partial):
    rows = q.shape[0]
    seq = k.shape[0]
    blk = BLK
    pairs = rows * (seq + blk) // 2 * per
    row = pl.BlockSpec((blk, per * head), lambda i: (i, 0))
    once = lambda n: pl.BlockSpec((n, head), lambda i: (0, 0), pipeline_mode=pl.Buffered(1))
    anywhere = pl.BlockSpec(memory_space=pl.ANY)
    dq_shape = jax.ShapeDtypeStruct((rows, per * head), BF16)
    if z == 0:
        out_specs = [row, anywhere, anywhere]
        out_shape = [dq_shape, jax.ShapeDtypeStruct((seq, head), F32), jax.ShapeDtypeStruct((seq, head), F32)]
    else:
        out_specs = [row, once(seq), once(seq)]
        out_shape = [dq_shape, jax.ShapeDtypeStruct((seq, head), BF16), jax.ShapeDtypeStruct((seq, head), BF16)]
    return pl.pallas_call(
        functools.partial(attn_bwd_kernel, z, per, head, blk),
        name='attn_bwd',
        grid=(rows // blk,),
        in_specs=[row, row, row, pl.BlockSpec((per, blk), lambda i: (0, i)), once(seq), once(seq),
                  pl.BlockSpec((head, seq), lambda i: (0, 0), pipeline_mode=pl.Buffered(1))] + [anywhere] * len(partial),
        out_specs=out_specs,
        out_shape=out_shape,
        scratch_shapes=[pltpu.VMEM((seq, head), F32), pltpu.VMEM((seq, head), F32), pltpu.VMEM((per, head, blk), F32),
                        pltpu.VMEM((per * blk, head), BF16), pltpu.VMEM((per * blk, head), BF16), pltpu.VMEM((1, per * blk), F32),
                        pltpu.SemaphoreType.DMA((2,))],
        compiler_params=pltpu.CompilerParams(dimension_semantics=('arbitrary',), vmem_limit_bytes=VMEM_LIMIT),
        cost_estimate=pl.CostEstimate(flops=10 * pairs * head, bytes_accessed=rows * head * 8 * per + seq * head * 16, transcendentals=pairs),
    )(q, d_out, o, lse, k, v, k_t, *partial)


def solution(mesh):
    group = mesh.shape['sp']

    def gather(arr, axis=0):
        return lax.all_gather(arr, 'sp', axis=axis, tiled=True)

    def exchange(arr):
        return lax.all_to_all(arr.reshape(group, -1, arr.shape[1]), 'sp', 0, 0, tiled=True)

    def device_step(x_in, dy_in, positions, w_q, w_k, w_v, w_o, w_pre, w_post, q_norm, k_norm):
        _, _, width = x_in.shape
        head = q_norm.shape[0]
        n_q = w_q.shape[1] // head // group
        n_k = w_k.shape[1] // head // group
        per = n_q // n_k
        me = lax.axis_index('sp')
        halves = [slice(z * BLK, (z + 1) * BLK) for z in range(2)]
        dy_half = [dy_in[0, rows] for rows in halves]
        x_half = [x_in[0, rows] for rows in halves]

        def mine(w, n, axis):
            return lax.dynamic_slice_in_dim(w, me * n * head, n * head, axis)

        x_f32, normed, pre_pull, normed_all = [], [], [], []
        for z in range(2):
            if z == 1:
                x_half[1], normed[0] = lax.optimization_barrier((x_half[1], normed[0]))
                normed_all.append(gather(normed[0]))
            x_f32.append(x_half[z].astype(F32))
            out, pull = jax.vjp(pre_norm, x_f32[z], w_pre)
            normed.append(out)
            pre_pull.append(pull)
        normed[0], positions = lax.optimization_barrier((normed[0], positions))
        normed[1], pos_all = lax.optimization_barrier((normed[1], gather(positions)))
        cosines, sines = rope_tables(pos_all, head)
        w_mine = jnp.concatenate([mine(w_q, n_q, 1), mine(w_k, n_k, 1), mine(w_v, n_k, 1)], axis=1)
        qn = q_norm[None, :]
        kn = k_norm[None, :]
        local = [dot(normed[1], w, NN).astype(BF16).reshape(BLK, group, -1) for w in (w_k, w_v, w_q)]
        local = jnp.concatenate([local[2], local[0], local[1]], axis=2).swapaxes(0, 1)
        local = lax.all_to_all(local, 'sp', 0, 0, tiled=True)
        w_mine, cosines, sines = lax.optimization_barrier((w_mine, cosines, sines))
        qkv_0 = dot(normed_all[0], w_mine, NN).astype(BF16)
        local, qkv_0, to_gather = lax.optimization_barrier((local, qkv_0, normed[1]))
        qkv = [qkv_0, local.reshape(group * BLK, -1)]
        q_all, kv = [], ()
        for z in range(2):
            q, *kv = rope_fwd(z, qkv[z], cosines, sines, qn, kn, n_q, n_k, head, kv)
            q_all.append(q)
        k_all, v_all, k_t, v_t = kv
        normed_all.append(gather(to_gather))

        w_o3 = w_o.reshape(group, n_q * head, width)
        o_all, lse, y_out, dy_f32, d_proj_all, dw_post = [], [], [], [], [], []
        for z in range(2):
            o, row_lse = attn_fwd(z, q_all[z], k_all, v_t, per, head)
            o_all.append(o)
            lse.append(row_lse)
        o_mine = [exchange(o_all[0])]
        o_mine[0], o_all[1] = lax.optimization_barrier((o_mine[0], o_all[1]))
        o_mine.append(exchange(o_all[1]))
        for z in range(2):
            proj = jnp.einsum('gtn,gnd->td', o_mine[z], w_o3, preferred_element_type=F32).astype(BF16)
            post, post_pull = jax.vjp(post_norm, proj, w_post)
            y_out.append((x_f32[z] + post).astype(BF16))
            dy_f32.append(dy_half[z].astype(F32))
            d_proj, dw = post_pull(dy_f32[z])
            dw_post.append(dw)
            if z == 0:
                dy_half[1], d_proj, o_mine[1], normed_all[1] = lax.optimization_barrier((dy_half[1], d_proj, o_mine[1], normed_all[1]))
            d_proj_all.append(gather(d_proj))

        wo_mine = mine(w_o, n_q, 0)
        do_0 = dot(d_proj_all[0], wo_mine, NT).astype(BF16)
        dq_0, *partial = attn_bwd(0, q_all[0], do_0, o_all[0], lse[0], k_all, v_all, k_t, per, head, ())
        dq_proj_0, gq_0 = rope_bwd(0, dq_0, (), qkv[0], 0, cosines, sines, qn, n_q, head)
        do_1 = dot(d_proj_all[1], wo_mine, NT).astype(BF16)
        dw_o = (dot(o_all[0], d_proj_all[0], TN) + dot(o_all[1], d_proj_all[1], TN)).astype(BF16)
        dq_flat_0 = exchange(dq_proj_0)
        do_1, dw_o, dq_flat_0, partial = lax.optimization_barrier((do_1, dw_o, dq_flat_0, partial))
        dw_o = gather(dw_o)
        dq_1, dk_all, dv_all = attn_bwd(1, q_all[1], do_1, o_all[1], lse[1], k_all, v_all, k_t, per, head, partial)
        dq_proj_1, gq_1 = rope_bwd(1, dq_1, (), qkv[1], 0, cosines, sines, qn, n_q, head)
        dq_flat = [dq_flat_0, exchange(dq_proj_1)]

        def weight_grad(grads):
            return (dot(normed_all[0], grads[0], TN) + dot(normed_all[1], grads[1], TN)).astype(BF16)

        dw_q = weight_grad((dq_proj_0, dq_proj_1))
        dw_q, dw_o, dq_flat[1], dk_all, dv_all = lax.optimization_barrier((dw_q, dw_o, dq_flat[1], dk_all, dv_all))
        dw_q = gather(dw_q, 1)
        dkv, gk = [], []
        for z in range(2):
            out, sums = rope_bwd(z, dk_all, (dv_all,), qkv[z], n_q, cosines, sines, kn, n_k, head)
            dkv.append(out)
            gk.append(sums)
        dkv_flat = [exchange(dkv[0])]
        dw_kv = weight_grad(dkv)
        dw_kv, dkv_flat[0], dkv[1] = lax.optimization_barrier((dw_kv, dkv_flat[0], dkv[1]))
        top = width // 2
        dw_kv_top = gather(dw_kv[:top], 1)
        dw_kv_rest = gather(dw_kv[top:], 1)
        dkv_flat.append(exchange(dkv[1]))
        dw_o = place(dw_o)

        def back(flat, w):
            return jnp.einsum('gtn,dgn->td', flat, w.reshape(width, group, -1), preferred_element_type=F32)

        dx_out, dw_pre = [], []
        for z in range(2):
            dk_flat = dkv_flat[z][:, :, :n_k * head]
            dv_flat = dkv_flat[z][:, :, n_k * head:]
            d_normed = (back(dq_flat[z], w_q) + back(dk_flat, w_k) + back(dv_flat, w_v)).astype(BF16)
            dx_norm, dw = pre_pull[z](d_normed)
            dw_pre.append(dw)
            dx_out.append((dy_f32[z] + dx_norm).astype(BF16))
        dw_pre = dw_pre[0] + dw_pre[1]
        dw_pre, dw_o = lax.optimization_barrier((dw_pre, dw_o))
        sums = lax.psum((dw_pre, dw_post[0] + dw_post[1], jnp.sum(gq_0 + gq_1, axis=0), jnp.sum(gk[0] + gk[1], axis=0)), 'sp')
        dw_q, sums = lax.optimization_barrier((dw_q, sums))
        dw_k, dw_v = split_pairs(dw_kv_rest, n_k * head, width, top, split_pairs(dw_kv_top, n_k * head, width, 0, ()))
        return (jnp.concatenate(y_out)[None], jnp.concatenate(dx_out)[None], place(dw_q), dw_k, dw_v, dw_o, sums[0], sums[1], sums[2], sums[3])

    token_spec = P('dp', 'sp', None)
    return jax.shard_map(device_step, mesh=mesh,
                         in_specs=(token_spec, token_spec, P(('dp', 'sp')), P(None, None), P(None, None), P(None, None), P(None, None), P(None), P(None), P(None), P(None)),
                         out_specs=(token_spec, token_spec, P('dp', None), P('dp', None), P('dp', None), P('dp', None), P('dp'), P('dp'), P('dp'), P('dp')),
                         check_vma=False)
```

```python
import functools
import jax
import jax.numpy as jnp
from jax import lax
from jax.experimental import pallas as pl
from jax.experimental.pallas import tpu as pltpu
from jax.sharding import PartitionSpec as P

EPS = 1e-6
ROPE_BASE = 1000000.0
ROPE_SCALE = 8.0
NEG_BIG = -1e30
LOG2E = 1.4426950408889634
F32 = jnp.float32
BF16 = jnp.bfloat16
NT = (((1,), (1,)), ((), ()))
NN = (((1,), (0,)), ((), ()))
TN = (((0,), (0,)), ((), ()))
VMEM_LIMIT = 60 * 1024 * 1024


def dot(a, b, dims):
    return lax.dot_general(a, b, dims, preferred_element_type=F32)


def rms_scale(x_f32, weight):
    inv_rms = lax.rsqrt(jnp.mean(x_f32 * x_f32, axis=-1, keepdims=True) + EPS)
    return x_f32 * inv_rms * (1.0 + weight)


def pre_norm(x_f32, weight):
    return rms_scale(x_f32, weight).astype(BF16)


def post_norm(proj, weight):
    return rms_scale(proj.astype(F32), weight)


def rope_tables(positions, head):
    half_dim = head // 2
    inv_freq = ROPE_BASE ** (-jnp.arange(half_dim, dtype=F32) * 2.0 / head)
    angles = (positions.astype(F32) / ROPE_SCALE)[:, None] * inv_freq[None, :]
    return jnp.cos(angles), jnp.sin(angles)


def rope_fwd_kernel(n_q, n_k, head, x_ref, cos_ref, sin_ref, wq_ref, wk_ref, *refs):
    q_ref, k_ref, v_ref, kt_ref, vt_ref = refs[-5:]
    half = head // 2
    cosines = cos_ref[...]
    sines = sin_ref[...]
    for h in range(n_q + n_k):
        x = x_ref[:, h * head:(h + 1) * head].astype(F32)
        w_ref, out_ref, at = (wq_ref, q_ref, h) if h < n_q else (wk_ref, k_ref, h - n_q)
        normed = rms_scale(x, w_ref[...])
        first = normed[:, :half]
        second = normed[:, half:]
        out_ref[:, at * head:at * head + half] = (first * cosines - second * sines).astype(BF16)
        out_ref[:, at * head + half:(at + 1) * head] = (second * cosines + first * sines).astype(BF16)
    v_ref[...] = x_ref[:, (n_q + n_k) * head:]
    kt_ref[...] = k_ref[...].T
    vt_ref[...] = v_ref[...].T


def rope_fwd(z, qkv, cosines, sines, w_qn, w_kn, n_q, n_k, head, kv_so_far):
    seq = cosines.shape[0]
    blk = BLK
    half = head // 2
    row = lambda width: pl.BlockSpec((blk, width), lambda i: (i, 0))
    placed = lambda width: pl.BlockSpec((blk, width), lambda i: (2 * i + z, 0))
    whole = pl.BlockSpec((1, head), lambda i: (0, 0))
    kv_shape = jax.ShapeDtypeStruct((seq, n_k * head), BF16)
    t_shape = jax.ShapeDtypeStruct((n_k * head, seq), BF16)
    t_placed = pl.BlockSpec((n_k * head, blk), lambda i: (0, 2 * i + z))
    return pl.pallas_call(
        functools.partial(rope_fwd_kernel, n_q, n_k, head),
        name='rope_fwd',
        grid=(qkv.shape[0] // blk,),
        in_specs=[row((n_q + 2 * n_k) * head), placed(half), placed(half), whole, whole] + [pl.BlockSpec(memory_space=pl.ANY)] * len(kv_so_far),
        out_specs=[row(n_q * head), placed(n_k * head), placed(n_k * head), t_placed, t_placed],
        out_shape=[jax.ShapeDtypeStruct((qkv.shape[0], n_q * head), BF16), kv_shape, kv_shape, t_shape, t_shape],
        input_output_aliases={5: 1, 6: 2, 7: 3, 8: 4} if kv_so_far else {},
        compiler_params=pltpu.CompilerParams(dimension_semantics=('arbitrary',)),
        cost_estimate=pl.CostEstimate(flops=qkv.size * 40, bytes_accessed=qkv.size * 4 + seq * head * 2, transcendentals=0),
    )(qkv, cosines, sines, w_qn, w_kn, *kv_so_far)


def rope_bwd_kernel(n, head, d_ref, x_ref, cos_ref, sin_ref, w_ref, *refs):
    out_ref, sum_ref = refs[-2:]
    half = head // 2
    cosines = cos_ref[...]
    sines = sin_ref[...]

    @pl.when(pl.program_id(0) == 0)
    def _():
        sum_ref[...] = jnp.zeros_like(sum_ref)

    for h in range(n):
        x = x_ref[:, h * head:(h + 1) * head].astype(F32)
        d_first = d_ref[:, h * head:h * head + half].astype(F32)
        d_second = d_ref[:, h * head + half:(h + 1) * head].astype(F32)
        g = jnp.concatenate([d_first * cosines + d_second * sines, d_second * cosines - d_first * sines], axis=1)
        inv_rms = lax.rsqrt(jnp.mean(x * x, axis=-1, keepdims=True) + EPS)
        x_hat = x * inv_rms
        sum_ref[...] += jnp.sum((g * x_hat).reshape(x.shape[0] // 8, 8, head), axis=0)
        gw = g * (1.0 + w_ref[...])
        out = inv_rms * (gw - x_hat * jnp.mean(gw * x_hat, axis=-1, keepdims=True))
        out_ref[:, h * head:(h + 1) * head] = out.astype(BF16)
    if len(refs) == 3:
        out_ref[:, n * head:] = refs[0][...]


def rope_bwd(z, grad, beside, qkv, lane_block, cosines, sines, w_n, n, head):
    blk = BLK
    half = head // 2
    row = lambda width: pl.BlockSpec((blk, width), lambda i: (i, 0))
    placed = lambda width: pl.BlockSpec((blk, width), lambda i: (2 * i + z, 0))
    rows = qkv.shape[0]
    lanes = n * head + sum(b.shape[1] for b in beside)
    return pl.pallas_call(
        functools.partial(rope_bwd_kernel, n, head),
        name='rope_bwd',
        grid=(rows // blk,),
        in_specs=[placed(n * head) if beside else row(n * head), pl.BlockSpec((blk, n * head), lambda i: (i, lane_block)),
                  placed(half), placed(half), pl.BlockSpec((1, head), lambda i: (0, 0))] + [placed(b.shape[1]) for b in beside],
        out_specs=[row(lanes), pl.BlockSpec((8, head), lambda i: (0, 0))],
        out_shape=[jax.ShapeDtypeStruct((rows, lanes), BF16), jax.ShapeDtypeStruct((8, head), F32)],
        compiler_params=pltpu.CompilerParams(dimension_semantics=('arbitrary',)),
        cost_estimate=pl.CostEstimate(flops=rows * n * head * 60, bytes_accessed=rows * n * head * 6 + rows * head * 4, transcendentals=0),
    )(grad, qkv, cosines, sines, w_n, *beside)


def copy_kernel(x_ref, o_ref):
    o_ref[...] = x_ref[...]


def place(x):
    rows = 256
    spec = pl.BlockSpec((rows, x.shape[1]), lambda i: (i, 0))
    return pl.pallas_call(
        copy_kernel,
        name='place',
        grid=(x.shape[0] // rows,),
        in_specs=[spec],
        out_specs=spec,
        out_shape=jax.ShapeDtypeStruct(x.shape, x.dtype),
        compiler_params=pltpu.CompilerParams(dimension_semantics=('arbitrary',)),
        cost_estimate=pl.CostEstimate(flops=x.size * 16, bytes_accessed=4 * x.size, transcendentals=0),
    )(x)


def split_kernel(x_ref, *refs):
    a_ref, b_ref = refs[-2:]
    a_ref[...] = x_ref[:, :a_ref.shape[1]]
    b_ref[...] = x_ref[:, a_ref.shape[1]:]


def split_pairs(x, lanes, out_rows, first_row, so_far):
    rows = x.shape[0] // 3
    parts = x.shape[1] // (2 * lanes)
    out = pl.BlockSpec((rows, lanes), lambda i, g: (i + first_row // rows, g))
    shape = jax.ShapeDtypeStruct((out_rows, parts * lanes), x.dtype)
    return pl.pallas_call(
        split_kernel,
        name='split_pairs',
        grid=(3, parts),
        in_specs=[pl.BlockSpec((rows, 2 * lanes), lambda i, g: (i, g))] + [pl.BlockSpec(memory_space=pl.ANY)] * len(so_far),
        out_specs=[out, out],
        out_shape=[shape, shape],
        input_output_aliases={1: 0, 2: 1} if so_far else {},
        compiler_params=pltpu.CompilerParams(dimension_semantics=('arbitrary', 'arbitrary')),
        cost_estimate=pl.CostEstimate(flops=x.size * 16, bytes_accessed=4 * x.size, transcendentals=0),
    )(x, *so_far)


BLK = 512


def attn_fwd_kernel(z, per, head, blk, q_ref, k_ref, vt_ref, o_ref, lse_ref, m_sc, l_sc, acc_sc, s_even, s_odd):
    i = pl.program_id(0)
    c = LOG2E * head ** -0.5
    m_sc[...] = jnp.full_like(m_sc, -jnp.inf)
    l_sc[...] = jnp.zeros_like(l_sc)
    acc_sc[...] = jnp.zeros_like(acc_sc)

    def scores(j, s_ref):
        k = k_ref[pl.ds(pl.multiple_of(j * blk, blk), blk), :]
        for h in range(per):
            s_ref[h] = dot(k, q_ref[:, h * head:(h + 1) * head], NT)

    def update(j, s_ref, masked):
        v_t = vt_ref[:, pl.ds(pl.multiple_of(j * blk, blk), blk)]
        for h in range(per):
            s = s_ref[h]
            if masked:
                kv_ids = lax.broadcasted_iota(jnp.int32, s.shape, 0)
                q_ids = lax.broadcasted_iota(jnp.int32, s.shape, 1)
                s = jnp.where(q_ids >= kv_ids, s, NEG_BIG)
            t = s * c
            m_prev = m_sc[h]
            m_new = jnp.maximum(m_prev, jnp.max(t, axis=0, keepdims=True))
            m_sc[h] = m_new
            p = jnp.exp2(t - m_new)
            alpha = jnp.exp2(m_prev - m_new)
            l_sc[h] = l_sc[h] * alpha + jnp.sum(p.reshape(blk // 8, 8, blk), axis=0)
            acc_sc[h] = acc_sc[h] * alpha + dot(v_t, p.astype(BF16), NN)

    scores(0, s_even)

    @pl.loop(0, i)
    def _(j):
        scores(2 * j + 1, s_odd)
        update(2 * j, s_even, False)
        scores(2 * j + 2, s_even)
        update(2 * j + 1, s_odd, False)

    if z == 0:
        update(2 * i, s_even, True)
    else:
        scores(2 * i + 1, s_odd)
        update(2 * i, s_even, False)
        update(2 * i + 1, s_odd, True)
    for h in range(per):
        total = jnp.sum(l_sc[h], axis=0, keepdims=True)
        o_ref[:, h * head:(h + 1) * head] = (acc_sc[h] / total).T.astype(BF16)
        lse_ref[h:h + 1, :] = m_sc[h] + jnp.log2(total)


def attn_fwd(z, q, k, v_t, per, head):
    rows = q.shape[0]
    seq = k.shape[0]
    blk = BLK
    pairs = rows * (seq + blk) // 2 * per
    row = pl.BlockSpec((blk, per * head), lambda i: (i, 0))
    whole = pl.BlockSpec((seq, head), lambda i: (0, 0), pipeline_mode=pl.Buffered(1))
    return pl.pallas_call(
        functools.partial(attn_fwd_kernel, z, per, head, blk),
        name='attn_fwd',
        grid=(rows // blk,),
        in_specs=[row, whole, pl.BlockSpec((head, seq), lambda i: (0, 0), pipeline_mode=pl.Buffered(1))],
        out_specs=[row, pl.BlockSpec((per, blk), lambda i: (0, i))],
        out_shape=[jax.ShapeDtypeStruct((rows, per * head), BF16), jax.ShapeDtypeStruct((per, rows), F32)],
        scratch_shapes=[pltpu.VMEM((per, 1, blk), F32), pltpu.VMEM((per, 8, blk), F32), pltpu.VMEM((per, head, blk), F32),
                        pltpu.VMEM((per, blk, blk), F32), pltpu.VMEM((per, blk, blk), F32)],
        compiler_params=pltpu.CompilerParams(dimension_semantics=('arbitrary',), vmem_limit_bytes=VMEM_LIMIT),
        cost_estimate=pl.CostEstimate(flops=4 * pairs * head, bytes_accessed=rows * head * 4 * per + seq * head * 4, transcendentals=pairs),
    )(q, k, v_t)


def attn_bwd_kernel(z, per, head, blk, q_ref, do_ref, o_ref, lse_ref, k_ref, v_ref, kt_ref, *refs):
    if z == 0:
        dq_ref, dk_ref, dv_ref, dk_acc, dv_acc, dq_acc, q_sc, do_sc, delta_sc, sems = refs
    else:
        dk_in, dv_in, dq_ref, dk_ref, dv_ref, dk_acc, dv_acc, dq_acc, q_sc, do_sc, delta_sc, sems = refs
    i = pl.program_id(0)
    last = pl.num_programs(0) - 1
    scale = head ** -0.5
    c = LOG2E * scale

    @pl.when(i == 0)
    def _():
        if z == 0:
            dk_acc[...] = jnp.zeros_like(dk_acc)
            dv_acc[...] = jnp.zeros_like(dv_acc)
        else:
            loads = [pltpu.make_async_copy(dk_in, dk_acc, sems.at[0]), pltpu.make_async_copy(dv_in, dv_acc, sems.at[1])]
            for load in loads:
                load.start()
            for load in loads:
                load.wait()

    for h in range(per):
        lanes = slice(h * head, (h + 1) * head)
        rows = slice(h * blk, (h + 1) * blk)
        q_sc[rows, :] = q_ref[:, lanes]
        do_sc[rows, :] = do_ref[:, lanes]
        prod = do_ref[:, lanes].astype(F32) * o_ref[:, lanes].astype(F32)
        delta = jnp.broadcast_to(jnp.sum(prod, axis=1, keepdims=True), (blk, 128))
        delta_sc[:, rows] = delta.T[0:1, :]

    def step(j, diag):
        at = pl.ds(pl.multiple_of(j * blk, blk), blk)
        k = k_ref[at, :]
        v = v_ref[at, :]
        k_t = kt_ref[:, at]
        dvs = []
        dks = []
        dqs = []
        for h in range(per):
            rows = slice(h * blk, (h + 1) * blk)
            q = q_sc[rows, :]
            d_out = do_sc[rows, :]
            s = dot(k, q, NT)
            p = jnp.exp2(s * c - lse_ref[h:h + 1, :])
            if diag:
                kv_ids = lax.broadcasted_iota(jnp.int32, s.shape, 0)
                q_ids = lax.broadcasted_iota(jnp.int32, s.shape, 1)
                p = jnp.where(q_ids >= kv_ids, p, 0.0)
            dp = dot(v, d_out, NT)
            ds = (p * (dp - delta_sc[:, rows])).astype(BF16)
            dvs.append(dot(p.astype(BF16), d_out, NN))
            dks.append(dot(ds, q, NN))
            dqs.append(dot(k_t, ds, NN))
        dv_acc[at, :] += functools.reduce(jnp.add, dvs)
        dk_acc[at, :] += functools.reduce(jnp.add, dks)
        for h in range(per):
            if diag:
                dq_acc[h] = dqs[h]
            else:
                dq_acc[h] += dqs[h]

    step(2 * i + z, True)

    @pl.loop(0, 2 * i + z)
    def _(j):
        step(j, False)

    for h in range(per):
        dq_ref[:, h * head:(h + 1) * head] = (dq_acc[h] * scale).T.astype(BF16)

    @pl.when(i == last)
    def _():
        if z == 0:
            stores = [pltpu.make_async_copy(dk_acc, dk_ref, sems.at[0]), pltpu.make_async_copy(dv_acc, dv_ref, sems.at[1])]
            for store in stores:
                store.start()
            for store in stores:
                store.wait()
        else:
            @pl.loop(0, dk_acc.shape[0] // blk)
            def _(j):
                at = pl.ds(pl.multiple_of(j * blk, blk), blk)
                dk_ref[at, :] = (dk_acc[at, :] * scale).astype(BF16)
                dv_ref[at, :] = dv_acc[at, :].astype(BF16)


def attn_bwd(z, q, d_out, o, lse, k, v, k_t, per, head, partial):
    rows = q.shape[0]
    seq = k.shape[0]
    blk = BLK
    pairs = rows * (seq + blk) // 2 * per
    row = pl.BlockSpec((blk, per * head), lambda i: (i, 0))
    once = lambda n: pl.BlockSpec((n, head), lambda i: (0, 0), pipeline_mode=pl.Buffered(1))
    anywhere = pl.BlockSpec(memory_space=pl.ANY)
    dq_shape = jax.ShapeDtypeStruct((rows, per * head), BF16)
    if z == 0:
        out_specs = [row, anywhere, anywhere]
        out_shape = [dq_shape, jax.ShapeDtypeStruct((seq, head), F32), jax.ShapeDtypeStruct((seq, head), F32)]
    else:
        out_specs = [row, once(seq), once(seq)]
        out_shape = [dq_shape, jax.ShapeDtypeStruct((seq, head), BF16), jax.ShapeDtypeStruct((seq, head), BF16)]
    return pl.pallas_call(
        functools.partial(attn_bwd_kernel, z, per, head, blk),
        name='attn_bwd',
        grid=(rows // blk,),
        in_specs=[row, row, row, pl.BlockSpec((per, blk), lambda i: (0, i)), once(seq), once(seq),
                  pl.BlockSpec((head, seq), lambda i: (0, 0), pipeline_mode=pl.Buffered(1))] + [anywhere] * len(partial),
        out_specs=out_specs,
        out_shape=out_shape,
        scratch_shapes=[pltpu.VMEM((seq, head), F32), pltpu.VMEM((seq, head), F32), pltpu.VMEM((per, head, blk), F32),
                        pltpu.VMEM((per * blk, head), BF16), pltpu.VMEM((per * blk, head), BF16), pltpu.VMEM((1, per * blk), F32),
                        pltpu.SemaphoreType.DMA((2,))],
        compiler_params=pltpu.CompilerParams(dimension_semantics=('arbitrary',), vmem_limit_bytes=VMEM_LIMIT),
        cost_estimate=pl.CostEstimate(flops=10 * pairs * head, bytes_accessed=rows * head * 8 * per + seq * head * 16, transcendentals=pairs),
    )(q, d_out, o, lse, k, v, k_t, *partial)


def solution(mesh):
    group = mesh.shape['sp']

    def gather(arr, axis=0):
        return lax.all_gather(arr, 'sp', axis=axis, tiled=True)

    def exchange(arr):
        return lax.all_to_all(arr.reshape(group, -1, arr.shape[1]), 'sp', 0, 0, tiled=True)

    def device_step(x_in, dy_in, positions, w_q, w_k, w_v, w_o, w_pre, w_post, q_norm, k_norm):
        _, _, width = x_in.shape
        head = q_norm.shape[0]
        n_q = w_q.shape[1] // head // group
        n_k = w_k.shape[1] // head // group
        per = n_q // n_k
        me = lax.axis_index('sp')
        halves = [slice(z * BLK, (z + 1) * BLK) for z in range(2)]
        dy_half = [dy_in[0, rows] for rows in halves]
        x_half = [x_in[0, rows] for rows in halves]

        def mine(w, n, axis):
            return lax.dynamic_slice_in_dim(w, me * n * head, n * head, axis)

        x_f32, normed, pre_pull, normed_all = [], [], [], []
        for z in range(2):
            if z == 1:
                x_half[1], normed[0] = lax.optimization_barrier((x_half[1], normed[0]))
                normed_all.append(gather(normed[0]))
            x_f32.append(x_half[z].astype(F32))
            out, pull = jax.vjp(pre_norm, x_f32[z], w_pre)
            normed.append(out)
            pre_pull.append(pull)
        normed[0], positions = lax.optimization_barrier((normed[0], positions))
        normed[1], pos_all = lax.optimization_barrier((normed[1], gather(positions)))
        cosines, sines = rope_tables(pos_all, head)
        w_mine = jnp.concatenate([mine(w_q, n_q, 1), mine(w_k, n_k, 1), mine(w_v, n_k, 1)], axis=1)
        qn = q_norm[None, :]
        kn = k_norm[None, :]
        local = [dot(normed[1], w, NN).astype(BF16).reshape(BLK, group, -1) for w in (w_k, w_v, w_q)]
        local = jnp.concatenate([local[2], local[0], local[1]], axis=2).swapaxes(0, 1)
        local = lax.all_to_all(local, 'sp', 0, 0, tiled=True)
        w_mine, cosines, sines = lax.optimization_barrier((w_mine, cosines, sines))
        qkv_0 = dot(normed_all[0], w_mine, NN).astype(BF16)
        local, qkv_0, to_gather = lax.optimization_barrier((local, qkv_0, normed[1]))
        qkv = [qkv_0, local.reshape(group * BLK, -1)]
        q_all, kv = [], ()
        for z in range(2):
            q, *kv = rope_fwd(z, qkv[z], cosines, sines, qn, kn, n_q, n_k, head, kv)
            q_all.append(q)
        k_all, v_all, k_t, v_t = kv
        top = width // 2
        normed_left = gather(to_gather[:, :top])

        w_o3 = w_o.reshape(group, n_q * head, width)
        o_all, lse, y_out, dy_f32, d_proj_all, dw_post = [], [], [], [], [], []
        for z in range(2):
            o, row_lse = attn_fwd(z, q_all[z], k_all, v_t, per, head)
            o_all.append(o)
            lse.append(row_lse)
        o_mine = [exchange(o_all[0])]
        o_mine[0], o_all[1] = lax.optimization_barrier((o_mine[0], o_all[1]))
        o_mine.append(exchange(o_all[1]))
        for z in range(2):
            proj = jnp.einsum('gtn,gnd->td', o_mine[z], w_o3, preferred_element_type=F32).astype(BF16)
            post, post_pull = jax.vjp(post_norm, proj, w_post)
            y_out.append((x_f32[z] + post).astype(BF16))
            dy_f32.append(dy_half[z].astype(F32))
            d_proj, dw = post_pull(dy_f32[z])
            dw_post.append(dw)
            if z == 0:
                dy_half[1], d_proj, o_mine[1], normed_left = lax.optimization_barrier((dy_half[1], d_proj, o_mine[1], normed_left))
            d_proj_all.append(gather(d_proj))

        wo_mine = mine(w_o, n_q, 0)
        do_0 = dot(d_proj_all[0], wo_mine, NT).astype(BF16)
        dq_0, *partial = attn_bwd(0, q_all[0], do_0, o_all[0], lse[0], k_all, v_all, k_t, per, head, ())
        dq_0, to_gather = lax.optimization_barrier((dq_0, to_gather))
        normed_right = gather(to_gather[:, top:])
        dq_proj_0, gq_0 = rope_bwd(0, dq_0, (), qkv[0], 0, cosines, sines, qn, n_q, head)
        do_1 = dot(d_proj_all[1], wo_mine, NT).astype(BF16)
        dw_o = (dot(o_all[0], d_proj_all[0], TN) + dot(o_all[1], d_proj_all[1], TN)).astype(BF16)
        dq_flat_0 = exchange(dq_proj_0)
        do_1, dw_o, partial = lax.optimization_barrier((do_1, dw_o, partial))
        dw_o = gather(dw_o)
        dq_1, dk_all, dv_all = attn_bwd(1, q_all[1], do_1, o_all[1], lse[1], k_all, v_all, k_t, per, head, partial)
        dq_1, normed_right, dq_flat_0 = lax.optimization_barrier((dq_1, normed_right, dq_flat_0))
        dq_proj_1, gq_1 = rope_bwd(1, dq_1, (), qkv[1], 0, cosines, sines, qn, n_q, head)
        dq_flat = [dq_flat_0, exchange(dq_proj_1)]

        def weight_grad(grads):
            half_1 = jnp.concatenate([dot(normed_left, grads[1], TN), dot(normed_right, grads[1], TN)])
            return (dot(normed_all[0], grads[0], TN) + half_1).astype(BF16)

        dw_q = weight_grad((dq_proj_0, dq_proj_1))
        dw_q, dw_o, dq_flat[1], dk_all, dv_all = lax.optimization_barrier((dw_q, dw_o, dq_flat[1], dk_all, dv_all))
        dw_q = gather(dw_q, 1)
        dkv, gk = [], []
        for z in range(2):
            out, sums = rope_bwd(z, dk_all, (dv_all,), qkv[z], n_q, cosines, sines, kn, n_k, head)
            dkv.append(out)
            gk.append(sums)
        dkv_flat = [exchange(dkv[0])]
        dw_kv = weight_grad(dkv)
        dw_kv, dkv_flat[0], dkv[1] = lax.optimization_barrier((dw_kv, dkv_flat[0], dkv[1]))
        dw_kv_top = gather(dw_kv[:top], 1)
        dw_kv_rest = gather(dw_kv[top:], 1)
        dkv_flat.append(exchange(dkv[1]))
        dw_o = place(dw_o)

        def back(flat, w):
            return jnp.einsum('gtn,dgn->td', flat, w.reshape(width, group, -1), preferred_element_type=F32)

        dx_out, dw_pre = [], []
        for z in range(2):
            dk_flat = dkv_flat[z][:, :, :n_k * head]
            dv_flat = dkv_flat[z][:, :, n_k * head:]
            d_normed = (back(dq_flat[z], w_q) + back(dk_flat, w_k) + back(dv_flat, w_v)).astype(BF16)
            dx_norm, dw = pre_pull[z](d_normed)
            dw_pre.append(dw)
            dx_out.append((dy_f32[z] + dx_norm).astype(BF16))
        dw_pre = dw_pre[0] + dw_pre[1]
        dw_pre, dw_o = lax.optimization_barrier((dw_pre, dw_o))
        sums = lax.psum((dw_pre, dw_post[0] + dw_post[1], jnp.sum(gq_0 + gq_1, axis=0), jnp.sum(gk[0] + gk[1], axis=0)), 'sp')
        dw_q, sums = lax.optimization_barrier((dw_q, sums))
        dw_k, dw_v = split_pairs(dw_kv_rest, n_k * head, width, top, split_pairs(dw_kv_top, n_k * head, width, 0, ()))
        return (jnp.concatenate(y_out)[None], jnp.concatenate(dx_out)[None], place(dw_q), dw_k, dw_v, dw_o, sums[0], sums[1], sums[2], sums[3])

    token_spec = P('dp', 'sp', None)
    return jax.shard_map(device_step, mesh=mesh,
                         in_specs=(token_spec, token_spec, P(('dp', 'sp')), P(None, None), P(None, None), P(None, None), P(None, None), P(None), P(None), P(None), P(None)),
                         out_specs=(token_spec, token_spec, P('dp', None), P('dp', None), P('dp', None), P('dp', None), P('dp'), P('dp'), P('dp'), P('dp')),
                         check_vma=False)
```
